128 devices in a mesh: batch: 4 (over y_hi, core), tm: 8 (over x, y_lo), space: 4 (over z).
Axes of the slice: x: 4, y: 4 (y_hi: 2, y_lo: 2; y = y_hi * 2 + y_lo), z: 4, core: 2. Of those that a mesh axis runs over, the one named last changes fastest.
Arguments:
- clip_tokens: bfloat16 [4, 16, 32, 32, 1024], P('batch', None, 'space', 'tm'), may hold values from -6 to 6
- frame_order: int32 [4, 16], P('batch'), may hold values from 0 to 15, each once within a row
- row_reach: int32 [4, 16], P('batch', 'tm'), may hold values from 1 to 4
- spatial_gain: float32 [1024], replicated, may hold values from 0.1 to 1.9
- spatial_heads: bfloat16 [1024, 3072], replicated, may hold values from -2 to 2
- spatial_merge: bfloat16 [1024, 1024], replicated, may hold values from -0.1875 to 0.1875
- temporal_gain: float32 [1024], replicated, may hold values from 0.1 to 1.9
- temporal_heads: bfloat16 [1024, 3072], replicated, may hold values from -2 to 2
- temporal_merge: bfloat16 [1024, 1024], replicated, may hold values from -0.1875 to 0.1875
- cotangent: bfloat16 [4, 16, 32, 32, 1024], P('batch', 'tm', 'space'), may hold values from -0.059814453 to 0.059814453
Outputs:
- output: bfloat16 [4, 16, 32, 32, 1024], P('batch', 'tm', 'space')
- weight_grad: float32 [1024, 1024], P(('tm', 'space'))
The draws below stay inside these ranges and needn't reach their ends.
Inputs may be any that keep to these rules, and one draw needn't show every extreme that they name: Each row of frame_order names every number from 0 to 15 once.
All inputs are finite; a program needn't handle non-finite values.
Results may differ from the reference program's by a relative error of at most 0.025.
Values may be sent and summed in bfloat16 or wider, within the bound.
A program may use at most 128 MiB of HBM per device.

```python
import jax
import jax.numpy as jnp
from jax import lax

COLS = 32
HALO = 4
D = 1024
HEADS = 16
HEAD_DIM = 64
CLIPS = 4
FRAMES = 16
ROWS = 32


def projection_draw(key):
    key_one, key_two, key_three = jax.random.split(key, 3)
    plain_part = jnp.clip(jax.random.normal(key_one, (D, 3 * D), jnp.float32), -6.0, 6.0) * D ** (-0.5)
    return plain_part.astype(jnp.bfloat16)


def draw_spatial_heads(key, part):
    return projection_draw(jax.random.fold_in(key, 11))


def draw_temporal_heads(key, part):
    return projection_draw(jax.random.fold_in(key, 23))


def with_ends(drawn, own_key, smallest, high):
    index_at = [jax.random.randint(jax.random.fold_in(own_key, axis), (), 0, length) for axis, length in enumerate(drawn.shape)]
    longest = drawn.shape.index(max(drawn.shape))
    beside = index_at[:longest] + [(index_at[longest] + 1) % drawn.shape[longest]] + index_at[longest + 1:]
    return drawn.at[tuple(index_at)].set(smallest).at[tuple(beside)].set(high)


def block_levels(own_key, dims, cuts, low, high):
    factor_of, own = 1.0, jax.random.fold_in(own_key, 6)
    for dim, shards_of in cuts:
        steps = jnp.exp(jax.random.uniform(jax.random.fold_in(own, dim), (shards_of,), jnp.float32, low / len(cuts), high / len(cuts)))
        factor_of = factor_of * jnp.repeat(steps, dims[dim] // shards_of).reshape([-1 if axis == dim else 1 for axis in range(len(dims))])
    return factor_of


def gaussian(stream_key, extent, spread, bound, cuts=(), kind=jnp.bfloat16):
    entries = spread * jax.random.normal(stream_key, extent, jnp.float32)
    if cuts:
        entries = entries * block_levels(stream_key, extent, cuts, -0.22, 0.18)
    return jnp.clip(entries, -bound, bound).astype(kind)


def setup_inputs(seed: int = 0) -> dict:
    seeds = jax.random.split(jax.random.key(seed), 11)
    return {
        "clip_tokens": gaussian(seeds[0], (CLIPS, FRAMES, ROWS, COLS, D), 1.0, 6.0, ((0, 4), (2, 4), (3, 8))),
        "frame_order": jax.vmap(lambda own: jax.random.permutation(own, FRAMES))(jax.random.split(seeds[1], CLIPS)).reshape((CLIPS, FRAMES)).astype(jnp.int32),
        "row_reach": with_ends(jax.random.randint(seeds[2], (CLIPS, FRAMES), 1, HALO + 1), jax.random.fold_in(seeds[2], 1), 1, HALO).astype(jnp.int32),
        "spatial_gain": jnp.clip(1.0 + 0.18 * jax.random.normal(seeds[3], (D,), jnp.float32), 0.1, 1.9),
        "spatial_heads": draw_spatial_heads(jax.random.fold_in(seeds[10], 71), 0),
        "spatial_merge": gaussian(seeds[5], (D, D), D ** -0.5, 0.1875),
        "temporal_gain": jnp.clip(1.0 + 0.18 * jax.random.normal(seeds[6], (D,), jnp.float32), 0.1, 1.9),
        "temporal_heads": draw_temporal_heads(jax.random.fold_in(seeds[10], 71), 0),
        "temporal_merge": gaussian(seeds[8], (D, D), D ** -0.5, 0.1875),
        "cotangent": gaussian(seeds[9], (CLIPS, FRAMES, ROWS, COLS, D), 0.01, 0.059814453, ((0, 4), (1, 8), (2, 4))),
    }


floor_term = 0.5

def normalize(values, gain_vector):
    widened = values.astype(jnp.float32)
    scaled = widened * lax.rsqrt(lax.optimization_barrier(jnp.mean(widened * widened, axis=-1, keepdims=True)) + floor_term)
    return (scaled * gain_vector).astype(jnp.bfloat16)

def softmax_rounded(scores, allowed):
    masked = jnp.where(allowed, scores, -1e+30)
    top_score = lax.optimization_barrier(jnp.max(masked, axis=-1, keepdims=True))
    exponent = jnp.exp(masked - top_score)
    return (exponent / lax.optimization_barrier(jnp.sum(exponent, axis=-1, keepdims=True))).astype(jnp.bfloat16)

def spatial_frame(inputs):
    queries, keys_all, values_all, reach_now = inputs
    token_rows = jnp.arange(ROWS * COLS, dtype=jnp.int32) // COLS
    allowed = jnp.abs(token_rows[:, None] - token_rows[None, :]) <= reach_now
    query_heads = queries.astype(jnp.float32).reshape(-1, HEADS, HEAD_DIM)
    key_heads = keys_all.astype(jnp.float32).reshape(-1, HEADS, HEAD_DIM)
    value_heads = values_all.astype(jnp.float32).reshape(-1, HEADS, HEAD_DIM)
    scores = jnp.einsum('qhd,khd->hqk', query_heads, key_heads) * HEAD_DIM ** (-0.5)
    weights = softmax_rounded(scores, allowed[None])
    context = jnp.einsum('hqk,khd->qhd', weights.astype(jnp.float32), value_heads)
    return context.reshape(-1, D).astype(jnp.bfloat16)

def temporal_clip(queries, keys_all, values_all, order_row):
    query_heads = queries.astype(jnp.float32).reshape(FRAMES, -1, HEADS, HEAD_DIM)
    key_heads = keys_all.astype(jnp.float32).reshape(FRAMES, -1, HEADS, HEAD_DIM)
    value_heads = values_all.astype(jnp.float32).reshape(FRAMES, -1, HEADS, HEAD_DIM)
    scores = jnp.einsum('fthd,gthd->thfg', query_heads, key_heads) * HEAD_DIM ** (-0.5)
    allowed = order_row[None, :] <= order_row[:, None]
    weights = softmax_rounded(scores, allowed[None, None])
    context = jnp.einsum('thfg,gthd->fthd', weights.astype(jnp.float32), value_heads)
    return context.reshape(FRAMES, -1, D).astype(jnp.bfloat16)

def reference(clip_tokens, frame_order, row_reach, spatial_gain, spatial_heads, spatial_merge, temporal_gain, temporal_heads, temporal_merge, cotangent):
    tokens = ROWS * COLS

    def one_clip(running, inputs):
        frames_in, order_row, reach_row, cotangent_clip = inputs
        flat_input = frames_in.reshape(FRAMES, tokens, D)
        normed = normalize(flat_input, spatial_gain)
        projected = jnp.dot(normed, spatial_heads, preferred_element_type=jnp.float32).astype(jnp.bfloat16)
        spatial_context = lax.map(spatial_frame, (projected[..., :D], projected[..., D:2 * D], projected[..., 2 * D:], reach_row))
        middle = (flat_input.astype(jnp.float32) + jnp.dot(spatial_context, spatial_merge, preferred_element_type=jnp.float32)).astype(jnp.bfloat16)
        normed_two = normalize(middle, temporal_gain)
        projected_two = jnp.dot(normed_two, temporal_heads, preferred_element_type=jnp.float32).astype(jnp.bfloat16)
        temporal_context = temporal_clip(projected_two[..., :D], projected_two[..., D:2 * D], projected_two[..., 2 * D:], order_row)
        output_clip = (middle.astype(jnp.float32) + jnp.dot(temporal_context, temporal_merge, preferred_element_type=jnp.float32)).astype(jnp.bfloat16)
        gradient = running + lax.dot_general(temporal_context.reshape(-1, D), cotangent_clip.reshape(-1, D), (((0,), (0,)), ((), ())), preferred_element_type=jnp.float32)
        return (gradient, output_clip.reshape(FRAMES, ROWS, COLS, D))
    zero_grad = jnp.zeros((D, D), jnp.float32)
    weight_grad, output = lax.scan(one_clip, zero_grad, (clip_tokens, frame_order, row_reach, cotangent))
    return (output, weight_grad)
```

```python
import functools
import math

import jax
import jax.numpy as jnp
from jax import lax
from jax.experimental import pallas as pl
from jax.experimental.pallas import tpu as pltpu
from jax.sharding import PartitionSpec as P

D = 1024
HEAD_DIM = 64
FLOOR = 0.5
TM = 8
SP = 4
FR = 2
TB = 32
HB = 16
EXT = TB + 2 * HB
PAIR = 128
NEG = -1e30
QSCALE = HEAD_DIM**-0.5 * math.log2(math.e)
MESH = pl.DeviceIdType.MESH
F32 = jnp.float32
BF16 = jnp.bfloat16


def norm_rows(values, gain):
    x = values.astype(F32)
    x = x * lax.rsqrt(jnp.mean(x * x, axis=-1, keepdims=True) + FLOOR)
    return (x * gain).astype(BF16)


def head_masks(width):
    lane = lax.broadcasted_iota(jnp.int32, (1, width), 1)
    odd = lax.rem(lane // HEAD_DIM, 2).astype(F32)
    return (1.0 - odd) * QSCALE, odd * QSCALE


def iota(shape, dim):
    return lax.broadcasted_iota(jnp.int32, shape, dim)


def softmax_times(q, k, v, bias):
    s = lax.dot_general(q, k, (((1,), (1,)), ((), ())), preferred_element_type=F32)
    s = s + bias
    top = jnp.max(s, axis=-1, keepdims=True)
    p = jnp.exp2(s - top)
    total = jnp.sum(p, axis=-1, keepdims=True)
    o = jnp.dot(p.astype(BF16), v, preferred_element_type=F32)
    return o / total


def kernel(
    order_ref,
    reach_ref,
    gain1_ref,
    gain2_ref,
    x_hbm,
    cot_hbm,
    w1_hbm,
    m1_hbm,
    w2_hbm,
    m2_hbm,
    out_hbm,
    wg_ref,
    w1,
    m1,
    w2,
    m2,
    xbuf,
    xn,
    qe,
    qo,
    kv,
    sbias,
    ctx,
    cbuf,
    xpos,
    mid,
    xn2,
    qe2,
    qo2,
    kv2,
    tbias,
    ctx2,
    cot,
    obuf,
    pbuf,
    ra,
    sa,
    rb1,
    sb1,
    rb2,
    sb2,
    rb3,
    fin,
    lsem,
    xs,
    xr,
    hs,
    hr,
    cs,
    cr,
    ts,
    tr,
    os_,
    or_,
    as_,
    ar,
    b1s,
    b1r,
    b2s,
    b2r,
    b3s,
    b3r,
):
    me = lax.axis_index("tm")
    z = lax.axis_index("space")
    batch = lax.axis_index("batch")
    core = lax.rem(batch, 2)
    mate = batch + 1 - 2 * core
    far = lax.rem(batch + 2, 4)

    def peer(d):
        return lax.rem(me + d, TM)

    def zpeer(d):
        return lax.rem(z + d, SP)

    def rcopy(src, dst, send, recv, **where):
        return pltpu.make_async_remote_copy(
            src_ref=src, dst_ref=dst, send_sem=send, recv_sem=recv, device_id=where, device_id_type=MESH
        )

    loads = [
        pltpu.make_async_copy(w1_hbm, w1, lsem.at[0]),
        pltpu.make_async_copy(x_hbm, xpos, lsem.at[1]),
        pltpu.make_async_copy(m1_hbm, m1, lsem.at[2]),
        pltpu.make_async_copy(w2_hbm, w2, lsem.at[3]),
        pltpu.make_async_copy(m2_hbm, m2, lsem.at[4]),
        pltpu.make_async_copy(cot_hbm.at[me], cot.at[:, me], lsem.at[5]),
        pltpu.make_async_copy(x_hbm.at[0, me], xbuf.at[0, me, pl.ds(HB, TB)], lsem.at[6]),
        pltpu.make_async_copy(x_hbm.at[1, me], xbuf.at[1, me, pl.ds(HB, TB)], lsem.at[7]),
    ]
    for i in (6, 7, 0, 1, 2, 3, 4, 5):
        loads[i].start()

    barrier = pltpu.get_barrier_semaphore()
    for d in range(1, TM):
        pl.semaphore_signal(barrier, inc=1, device_id={"tm": peer(d)}, device_id_type=MESH)
    for d in range(1, SP):
        pl.semaphore_signal(barrier, inc=1, device_id={"space": zpeer(d)}, device_id_type=MESH)
    pl.semaphore_signal(barrier, inc=1, device_id={"batch": mate}, device_id_type=MESH)
    pl.semaphore_signal(barrier, inc=1, device_id={"batch": far}, device_id_type=MESH)
    pl.semaphore_wait(barrier, TM - 1 + SP - 1 + 2)

    pending = []

    tok = {}
    for f in range(FR):
        for d in range(1, TM):
            t = peer(d)
            cp = rcopy(x_hbm.at[f, t], xbuf.at[f, me, pl.ds(HB, TB)], xs.at[f, d], xr.at[f, d], tm=t)
            cp.start()
            tok[f, d] = cp
            pending.append(cp)
    cots = []
    for d in range(1, TM):
        t = peer(d)
        cp = rcopy(cot_hbm.at[t], cot.at[:, me], cs.at[d], cr.at[d], tm=t)
        cp.start()
        cots.append(cp)
        pending.append(cp)

    order_col = jnp.zeros((256, 1), jnp.int32)
    order_row = jnp.zeros((1, 256), jnp.int32)
    col_slot = iota((256, 1), 0) // 16
    row_slot = iota((1, 256), 1) // 16
    for f in range(FR):
        for s in range(TM):
            value = order_ref[0, s * FR + f]
            order_col = jnp.where(col_slot == f * TM + s, value, order_col)
            order_row = jnp.where(row_slot == f * TM + s, value, order_row)
    same = lax.rem(iota((256, 256), 0), 16) == lax.rem(iota((256, 256), 1), 16)
    tbias[...] = jnp.where(same & (order_row <= order_col), 0.0, NEG)
    key = iota((128, 384), 1)
    key_src = jnp.zeros((128, 384), jnp.int32)
    for n in range(1, TM):
        key_src = key_src + (key >= 48 * n).astype(jnp.int32)
    key_row = (key - 48 * key_src) // 4 - 4
    query_row = lax.rem(iota((128, 384), 0), 16) // 4
    distance = jnp.abs(key_row - query_row)
    for f in range(FR):
        for h in range(2):
            row = key_row + (z * 8 + 4 * h)
            keep = (distance <= reach_ref[0, f]) & (row >= 0) & (row < 8 * SP)
            sbias[f, h] = jnp.where(keep, 0.0, NEG)

    even_mask, odd_mask = head_masks(256)

    halo = {}

    def forward(f):
        for d in range(TM):
            if d == 0:
                loads[6 + f].wait()
            else:
                tok[f, d].wait_recv()
            s = lax.rem(me + TM - d, TM)
            up = rcopy(
                xbuf.at[f, s, pl.ds(HB, HB)],
                xbuf.at[f, s, pl.ds(HB + TB, HB)],
                hs.at[f, d, 0],
                hr.at[f, d, 0],
                space=zpeer(SP - 1),
            )
            down = rcopy(
                xbuf.at[f, s, pl.ds(TB, HB)],
                xbuf.at[f, s, pl.ds(0, HB)],
                hs.at[f, d, 1],
                hr.at[f, d, 1],
                space=zpeer(1),
            )
            up.start()
            down.start()
            halo[f, d] = (up, down)
            pending.extend((up, down))

    def project_own(f):
        xn[...] = norm_rows(xbuf[f, :, HB : HB + TB].reshape(TM * TB, D), gain1_ref[...])

        @pl.loop(0, 4)
        def _(n):
            at = pl.ds(pl.multiple_of(n * 256, 256), 256)
            acc = jnp.dot(xn[...], w1[:, at], preferred_element_type=F32)
            qe[:, :, at] = (acc * even_mask).astype(BF16).reshape(TM, TB, 256)
            qo[:, :, at] = (acc * odd_mask).astype(BF16).reshape(TM, TB, 256)

        @pl.loop(0, 8)
        def _(n):
            at = pl.ds(pl.multiple_of(n * 256, 256), 256)
            wat = pl.ds(pl.multiple_of(n * 256 + D, 256), 256)
            acc = jnp.dot(xn[...], w1[:, wat], preferred_element_type=F32)
            kv[:, HB : HB + TB, at] = acc.astype(BF16).reshape(TM, TB, 256)

    def project_halo(f):
        for d in range(TM):
            halo[f, d][0].wait_recv()
            halo[f, d][1].wait_recv()
        half = TM * HB
        xn[:half] = norm_rows(xbuf[f, :, :HB].reshape(half, D), gain1_ref[...])
        xn[half:] = norm_rows(xbuf[f, :, HB + TB :].reshape(half, D), gain1_ref[...])

        @pl.loop(0, 8)
        def _(n):
            at = pl.ds(pl.multiple_of(n * 256, 256), 256)
            wat = pl.ds(pl.multiple_of(n * 256 + D, 256), 256)
            acc = jnp.dot(xn[...], w1[:, wat], preferred_element_type=F32).astype(BF16)
            kv[:, :HB, at] = acc[:half].reshape(TM, HB, 256)
            kv[:, HB + TB :, at] = acc[half:].reshape(TM, HB, 256)

    lane_even = iota((1, PAIR), 1) < HEAD_DIM

    def attend(f):
        @pl.loop(0, 8)
        def _(n):
            at = pl.ds(pl.multiple_of(n * PAIR, PAIR), PAIR)
            vat = pl.ds(pl.multiple_of(n * PAIR + D, PAIR), PAIR)
            for h in range(2):
                rows = slice(h * HB, (h + 1) * HB)
                keys = slice(h * HB, h * HB + 3 * HB)
                k = kv[:, keys, at].reshape(384, PAIR)
                v = kv[:, keys, vat].reshape(384, PAIR)
                o = []
                for q in (qe, qo):
                    o.append(softmax_times(q[:, rows, at].reshape(128, PAIR), k, v, sbias[f, h]))
                both = jnp.where(lane_even, o[0], o[1]).astype(BF16)
                ctx[f, :, rows, at] = both.reshape(TM, HB, PAIR)

    back = {}

    def send_context(f):
        for d in range(1, TM):
            t = peer(d)
            cp = rcopy(ctx.at[f, t], cbuf.at[f, me], ts.at[f, d], tr.at[f, d], tm=t)
            cp.start()
            back[f, d] = cp
            pending.append(cp)

    forward(0)
    loads[0].wait()
    project_own(0)
    forward(1)
    project_halo(0)
    attend(0)
    send_context(0)
    project_own(1)
    project_halo(1)
    attend(1)
    send_context(1)

    loads[1].wait()
    loads[2].wait()
    loads[3].wait()

    for f in range(FR):
        cbuf[f, me] = ctx[f, me]
        for d in range(1, TM):
            back[f, d].wait_recv()

        @pl.loop(0, 4)
        def _(n):
            at = pl.ds(pl.multiple_of(n * 256, 256), 256)
            acc = jnp.dot(cbuf[f].reshape(TM * TB, D), m1[:, at], preferred_element_type=F32)
            acc = acc + xpos[f, :, :, at].reshape(TM * TB, 256).astype(F32)
            mid[f, :, at] = acc.astype(BF16)

        xn2[...] = norm_rows(mid[f], gain2_ref[...])

        @pl.loop(0, 4)
        def _(n):
            at = pl.ds(pl.multiple_of(n * 256, 256), 256)
            acc = jnp.dot(xn2[...], w2[:, at], preferred_element_type=F32)
            qe2[f, :, :, at] = (acc * even_mask).astype(BF16).reshape(TM, TB, 256)
            qo2[f, :, :, at] = (acc * odd_mask).astype(BF16).reshape(TM, TB, 256)

        @pl.loop(0, 8)
        def _(n):
            at = pl.ds(pl.multiple_of(n * 256, 256), 256)
            wat = pl.ds(pl.multiple_of(n * 256 + D, 256), 256)
            acc = jnp.dot(xn2[...], w2[:, wat], preferred_element_type=F32)
            kv2[f, :, :, at] = acc.astype(BF16).reshape(TM, TB, 256)

    loads[5].wait()
    for cp in cots:
        cp.wait_recv()

    first = []
    for g in range(4):

        @pl.loop(0, 2)
        def _(i):
            n = g * 2 + i
            at = pl.ds(pl.multiple_of(n * PAIR, PAIR), PAIR)
            vat = pl.ds(pl.multiple_of(n * PAIR + D, PAIR), PAIR)
            for b in range(2):
                rows = slice(b * 16, (b + 1) * 16)
                k = kv2[:, :, rows, at].reshape(256, PAIR)
                v = kv2[:, :, rows, vat].reshape(256, PAIR)
                o = []
                for q in (qe2, qo2):
                    o.append(softmax_times(q[:, :, rows, at].reshape(256, PAIR), k, v, tbias[...]))
                both = jnp.where(lane_even, o[0], o[1]).astype(BF16)
                ctx2[:, :, rows, at] = both.reshape(FR, TM, 16, PAIR)

        a = ctx2[:, :, :, g * 256 : (g + 1) * 256].reshape(FR * TM * TB, 256)

        @pl.loop(0, 4)
        def _(n):
            at = pl.ds(pl.multiple_of(n * 256, 256), 256)
            c = cot[:, :, :, at].reshape(FR * TM * TB, 256)
            acc = lax.dot_general(a, c, (((0,), (0,)), ((), ())), preferred_element_type=F32)
            pbuf[g * 2 : g * 2 + 2, :, :, :, at] = acc.astype(BF16).reshape(2, SP, 2, 16, 256)

        cp = rcopy(
            pbuf.at[pl.ds(g * 2, 2), :, 1 - core], ra.at[pl.ds(g * 2, 2)], as_.at[g], ar.at[g], batch=mate
        )
        cp.start()
        pending.append(cp)
        first.append(cp)
        if g > 0:
            reduce_rows(g - 1, first, pbuf, ra, sa, core)
            start_z(g - 1, sa, rb1, b1s, b1r, rcopy, zpeer, pending)
    loads[4].wait()
    outs = []
    for f in range(FR):

        @pl.loop(0, 4)
        def _(n):
            at = pl.ds(pl.multiple_of(n * 256, 256), 256)
            acc = jnp.dot(ctx2[f].reshape(TM * TB, D), m2[:, at], preferred_element_type=F32)
            acc = acc + mid[f, :, at].astype(F32)
            obuf[f, :, :, at] = acc.astype(BF16).reshape(TM, TB, 256)

        own = pltpu.make_async_copy(obuf.at[f, me], out_hbm.at[f, me], lsem.at[8 + f])
        own.start()
        outs.append(own)
        for d in range(1, TM):
            t = peer(d)
            cp = rcopy(obuf.at[f, t], out_hbm.at[f, me], os_.at[f, d], or_.at[f, d], tm=t)
            cp.start()
            outs.append(cp)
        if f == 0:
            reduce_rows(3, first, pbuf, ra, sa, core)
            start_z(3, sa, rb1, b1s, b1r, rcopy, zpeer, pending)

    last = []
    for g in range(4):
        for d in range(1, SP):
            rcopy(
                sa.at[pl.ds(g * 2, 2), zpeer(d)],
                rb1.at[d - 1, pl.ds(g * 2, 2)],
                b1s.at[g, d - 1],
                b1r.at[g, d - 1],
                space=zpeer(d),
            ).wait_recv()
        total = sa[pl.ds(g * 2, 2), z].astype(F32)
        for d in range(1, SP):
            total = total + rb1[d - 1, pl.ds(g * 2, 2)].astype(F32)
        sb1[pl.ds(g * 2, 2)] = total.astype(BF16)
    for d in range(1, TM):
        t = peer(d)
        cp = rcopy(sb1.at[t], rb2.at[d - 1], b2s.at[d], b2r.at[d], tm=t)
        cp.start()
        last.append(cp)
        pending.append(cp)
    total = sb1[me].astype(F32)
    for d in range(1, TM):
        last[d - 1].wait_recv()
        total = total + rb2[d - 1].astype(F32)
    sb2[...] = total.astype(BF16)
    cp = rcopy(sb2, rb3, b3s.at[0], b3r.at[0], batch=far)
    cp.start()
    cp.wait()
    fin[core] = sb2[...].astype(F32) + rb3[...].astype(F32)
    cp = rcopy(fin.at[core], fin.at[core], b3s.at[1], b3r.at[1], batch=mate)
    cp.start()
    cp.wait()
    wg_ref[...] = fin[...].reshape(32, D)

    for cp in pending:
        cp.wait_send()
    for cp in outs:
        cp.wait()


def reduce_rows(g, first, pbuf, ra, sa, core):
    first[g].wait_recv()
    rows = pl.ds(g * 2, 2)
    sa[rows] = (pbuf[rows, :, core].astype(F32) + ra[rows].astype(F32)).astype(BF16)


def start_z(g, sa, rb1, b1s, b1r, rcopy, zpeer, pending):
    rows = pl.ds(g * 2, 2)
    for d in range(1, SP):
        cp = rcopy(
            sa.at[rows, zpeer(d)], rb1.at[d - 1, rows], b1s.at[g, d - 1], b1r.at[g, d - 1], space=zpeer(d)
        )
        cp.start()
        pending.append(cp)


def per_device(
    clip_tokens,
    frame_order,
    row_reach,
    spatial_gain,
    spatial_heads,
    spatial_merge,
    temporal_gain,
    temporal_heads,
    temporal_merge,
    cotangent,
):
    tokens = clip_tokens.reshape(TM, FR, TB, D).transpose(1, 0, 2, 3)
    grads = cotangent.reshape(FR, 8, TM, 4, D).transpose(2, 0, 1, 3, 4).reshape(TM, FR, TB, D)
    dma = pltpu.SemaphoreType.DMA
    vm = pltpu.VMEM
    smem = pl.BlockSpec(memory_space=pltpu.SMEM)
    vmem = pl.BlockSpec(memory_space=pltpu.VMEM)
    anym = pl.BlockSpec(memory_space=pl.ANY)
    out, wg = pl.pallas_call(
        kernel,
        out_shape=[
            jax.ShapeDtypeStruct((FR, TM, TB, D), BF16),
            jax.ShapeDtypeStruct((32, D), F32),
        ],
        in_specs=[smem, smem, vmem, vmem] + [anym] * 6,
        out_specs=[anym, vmem],
        scratch_shapes=[
            vm((D, 3 * D), BF16),
            vm((D, D), BF16),
            vm((D, 3 * D), BF16),
            vm((D, D), BF16),
            vm((FR, TM, EXT, D), BF16),
            vm((TM * TB, D), BF16),
            vm((TM, TB, D), BF16),
            vm((TM, TB, D), BF16),
            vm((TM, EXT, 2 * D), BF16),
            vm((FR, 2, 128, 384), F32),
            vm((FR, TM, TB, D), BF16),
            vm((FR, TM, TB, D), BF16),
            vm((FR, TM, TB, D), BF16),
            vm((FR, TM * TB, D), BF16),
            vm((TM * TB, D), BF16),
            vm((FR, TM, TB, D), BF16),
            vm((FR, TM, TB, D), BF16),
            vm((FR, TM, TB, 2 * D), BF16),
            vm((256, 256), F32),
            vm((FR, TM, TB, D), BF16),
            vm((FR, TM, TB, D), BF16),
            vm((FR, TM, TB, D), BF16),
            vm((TM, SP, 2, 16, D), BF16),
            vm((TM, SP, 16, D), BF16),
            vm((TM, SP, 16, D), BF16),
            vm((SP - 1, TM, 16, D), BF16),
            vm((TM, 16, D), BF16),
            vm((TM - 1, 16, D), BF16),
            vm((16, D), BF16),
            vm((16, D), BF16),
            vm((2, 16, D), F32),
            dma((10,)),
            dma((FR, TM)),
            dma((FR, TM)),
            dma((FR, TM, 2)),
            dma((FR, TM, 2)),
            dma((TM,)),
            dma((TM,)),
            dma((FR, TM)),
            dma((FR, TM)),
            dma((FR, TM)),
            dma((FR, TM)),
            dma((4,)),
            dma((4,)),
            dma((4, SP - 1)),
            dma((4, SP - 1)),
            dma((TM,)),
            dma((TM,)),
            dma((2,)),
            dma((2,)),
        ],
        compiler_params=pltpu.CompilerParams(
            collective_id=0, has_side_effects=True, vmem_limit_bytes=62 * 1024 * 1024
        ),
    )(
        frame_order,
        row_reach,
        spatial_gain.reshape(1, D),
        temporal_gain.reshape(1, D),
        tokens,
        grads,
        spatial_heads,
        spatial_merge,
        temporal_heads,
        temporal_merge,
    )
    out = out.reshape(FR, TM, 8, 4, D).transpose(0, 2, 1, 3, 4).reshape(1, FR, 8, 32, D)
    return out, wg


def solution(mesh):
    in_specs = (
        P("batch", None, "space", "tm", None),
        P("batch", None),
        P("batch", "tm"),
        P(),
        P(),
        P(),
        P(),
        P(),
        P(),
        P("batch", "tm", "space", None, None),
    )
    out_specs = (P("batch", "tm", "space", None, None), P(("tm", "space"), None))
    return jax.shard_map(
        per_device, mesh=mesh, in_specs=in_specs, out_specs=out_specs, check_vma=False
    )
```

```python
import functools
import math

import jax
import jax.numpy as jnp
from jax import lax
from jax.experimental import pallas as pl
from jax.experimental.pallas import tpu as pltpu
from jax.sharding import PartitionSpec as P

D = 1024
HEAD_DIM = 64
FLOOR = 0.5
TM = 8
SP = 4
FR = 2
TB = 32
HB = 16
EXT = TB + 2 * HB
PAIR = 128
WIDE = 1024
GROUP = 2
NEG = -1e30
QSCALE = HEAD_DIM**-0.5 * math.log2(math.e)
MESH = pl.DeviceIdType.MESH
F32 = jnp.float32
BF16 = jnp.bfloat16


def unrolled(count):
    def run(body):
        for n in range(count):
            body(n)

    return run


def norm_rows(values, gain):
    x = values.astype(F32)
    x = x * lax.rsqrt(jnp.mean(x * x, axis=-1, keepdims=True) + FLOOR)
    return (x * gain).astype(BF16)


def head_masks(width):
    lane = lax.broadcasted_iota(jnp.int32, (1, width), 1)
    odd = lax.rem(lane // HEAD_DIM, 2).astype(F32)
    return (1.0 - odd) * QSCALE, odd * QSCALE


def iota(shape, dim):
    return lax.broadcasted_iota(jnp.int32, shape, dim)


def attend(chains):
    scores = [
        lax.dot_general(k, q, (((1,), (1,)), ((), ())), preferred_element_type=F32) + bias
        for q, k, _, bias in chains
    ]
    weights = []
    for s in scores:
        p = jnp.exp2(s - jnp.max(s, axis=0, keepdims=True))
        weights.append((p.astype(BF16), 1.0 / jnp.sum(p, axis=0, keepdims=True)))
    outputs = []
    for (q, _, v, _), (p, scale) in zip(chains, weights):
        count = q.shape[0] // 2
        o = lax.dot_general(v, p, (((0,), (0,)), ((), ())), preferred_element_type=F32) * scale
        both = jnp.where(iota((PAIR, count), 0) < HEAD_DIM, o[:, :count], o[:, count:])
        outputs.append(both.T.astype(BF16))
    return outputs


def kernel(
    order_ref,
    reach_ref,
    gain1_ref,
    gain2_ref,
    x_hbm,
    cot_hbm,
    w1_hbm,
    m1_hbm,
    w2_hbm,
    m2_hbm,
    out_hbm,
    wg_ref,
    w1,
    m1,
    w2,
    m2,
    xbuf,
    xn,
    qe,
    qo,
    kv,
    sbias,
    ctx,
    cbuf,
    xpos,
    mid,
    xn2,
    qe2,
    qo2,
    kv2,
    tbias,
    ctx2,
    cot,
    obuf,
    pbuf,
    ra,
    sa,
    rb1,
    sb1,
    rb2,
    sb2,
    rb3,
    lsem,
    xs,
    xr,
    hs,
    hr,
    cs,
    cr,
    ts,
    tr,
    os_,
    or_,
    as_,
    ar,
    b1s,
    b1r,
    b2s,
    b2r,
    b3s,
    b3r,
):
    me = lax.axis_index("tm")
    z = lax.axis_index("space")
    batch = lax.axis_index("batch")
    core = lax.rem(batch, 2)
    mate = batch + 1 - 2 * core
    others = (lax.rem(batch + 2, 4), mate, lax.rem(mate + 2, 4))

    def peer(d):
        return lax.rem(me + d, TM)

    def zpeer(d):
        return lax.rem(z + d, SP)

    def rcopy(src, dst, send, recv, **where):
        return pltpu.make_async_remote_copy(
            src_ref=src, dst_ref=dst, send_sem=send, recv_sem=recv, device_id=where, device_id_type=MESH
        )

    loads = [
        pltpu.make_async_copy(w1_hbm, w1, lsem.at[0]),
        pltpu.make_async_copy(x_hbm, xpos, lsem.at[1]),
        pltpu.make_async_copy(m1_hbm, m1, lsem.at[2]),
        pltpu.make_async_copy(w2_hbm, w2, lsem.at[3]),
        pltpu.make_async_copy(m2_hbm, m2, lsem.at[4]),
        pltpu.make_async_copy(cot_hbm.at[me], cot.at[:, me], lsem.at[5]),
        pltpu.make_async_copy(x_hbm.at[0, me], xbuf.at[0, me, pl.ds(HB, TB)], lsem.at[6]),
        pltpu.make_async_copy(x_hbm.at[1, me], xbuf.at[1, me, pl.ds(HB, TB)], lsem.at[7]),
    ]
    for i in (6, 7, 0, 1, 2, 3, 4, 5):
        loads[i].start()

    barrier = pltpu.get_barrier_semaphore()
    for d in range(1, TM):
        pl.semaphore_signal(barrier, inc=1, device_id={"tm": peer(d)}, device_id_type=MESH)
    for d in range(1, SP):
        pl.semaphore_signal(barrier, inc=1, device_id={"space": zpeer(d)}, device_id_type=MESH)
    for other in others:
        pl.semaphore_signal(barrier, inc=1, device_id={"batch": other}, device_id_type=MESH)
    with jax.named_scope("barrier"):
        pl.semaphore_wait(barrier, TM - 1 + SP - 1 + 3)

    pending = []

    tok = {}
    for f in range(FR):
        for d in range(1, TM):
            t = peer(d)
            cp = rcopy(x_hbm.at[f, t], xbuf.at[f, me, pl.ds(HB, TB)], xs.at[f, d], xr.at[f, d], tm=t)
            cp.start()
            tok[f, d] = cp
            pending.append(cp)
    cots = []

    def send_cotangent(f):
        for d in range(1, TM):
            t = peer(d)
            cp = rcopy(cot_hbm.at[t, f], cot.at[f, me], cs.at[f, d], cr.at[f, d], tm=t)
            cp.start()
            cots.append(cp)
            pending.append(cp)

    send_cotangent(0)

    order_key = jnp.zeros((256, 1), jnp.int32)
    order_query = jnp.zeros((1, 512), jnp.int32)
    key_slot = iota((256, 1), 0) // 16
    query_slot = lax.rem(iota((1, 512), 1) // 16, 16)
    for f in range(FR):
        for s in range(TM):
            value = order_ref[0, s * FR + f]
            order_key = jnp.where(key_slot == f * TM + s, value, order_key)
            order_query = jnp.where(query_slot == f * TM + s, value, order_query)
    same = lax.rem(iota((256, 512), 0), 16) == lax.rem(iota((256, 512), 1), 16)
    tbias[...] = jnp.where(same & (order_key <= order_query), 0.0, NEG)
    key = iota((384, 1), 0)
    key_src = jnp.zeros((384, 1), jnp.int32)
    for n in range(1, TM):
        key_src = key_src + (key >= 48 * n).astype(jnp.int32)
    key_row = (key - 48 * key_src) // 4 - 4
    query_row = lax.rem(iota((1, 256), 1), 16) // 4
    distance = jnp.abs(key_row - query_row)
    for f in range(FR):
        for h in range(2):
            row = key_row + (z * 8 + 4 * h)
            keep = (distance <= reach_ref[0, f]) & (row >= 0) & (row < 8 * SP)
            sbias[f, h] = jnp.where(keep, 0.0, NEG)

    even_mask, odd_mask = head_masks(WIDE)

    halo = {}

    def forward(f):
        for d in range(TM):
            if d == 0:
                loads[6 + f].wait()
            else:
                tok[f, d].wait_recv()
            s = lax.rem(me + TM - d, TM)
            up = rcopy(
                xbuf.at[f, s, pl.ds(HB, HB)],
                xbuf.at[f, s, pl.ds(HB + TB, HB)],
                hs.at[f, d, 0],
                hr.at[f, d, 0],
                space=zpeer(SP - 1),
            )
            down = rcopy(
                xbuf.at[f, s, pl.ds(TB, HB)],
                xbuf.at[f, s, pl.ds(0, HB)],
                hs.at[f, d, 1],
                hr.at[f, d, 1],
                space=zpeer(1),
            )
            up.start()
            down.start()
            halo[f, d] = (up, down)
            pending.extend((up, down))

    def project_own(f):
        xn[...] = norm_rows(xbuf[f, :, HB : HB + TB].reshape(TM * TB, D), gain1_ref[...])

        @unrolled(D // WIDE)
        def _(n):
            at = slice(n * WIDE, (n + 1) * WIDE)
            acc = jnp.dot(xn[...], w1[:, at], preferred_element_type=F32)
            qe[:, :, at] = (acc * even_mask).astype(BF16).reshape(TM, TB, WIDE)
            qo[:, :, at] = (acc * odd_mask).astype(BF16).reshape(TM, TB, WIDE)

        @unrolled(2 * D // WIDE)
        def _(n):
            at = slice(n * WIDE, (n + 1) * WIDE)
            wat = slice(n * WIDE + D, (n + 1) * WIDE + D)
            acc = jnp.dot(xn[...], w1[:, wat], preferred_element_type=F32)
            kv[:, HB : HB + TB, at] = acc.astype(BF16).reshape(TM, TB, WIDE)

    def project_halo(f):
        for d in range(TM):
            halo[f, d][0].wait_recv()
            halo[f, d][1].wait_recv()
        half = TM * HB
        xn[:half] = norm_rows(xbuf[f, :, :HB].reshape(half, D), gain1_ref[...])
        xn[half:] = norm_rows(xbuf[f, :, HB + TB :].reshape(half, D), gain1_ref[...])

        @unrolled(2 * D // WIDE)
        def _(n):
            at = slice(n * WIDE, (n + 1) * WIDE)
            wat = slice(n * WIDE + D, (n + 1) * WIDE + D)
            acc = jnp.dot(xn[...], w1[:, wat], preferred_element_type=F32).astype(BF16)
            kv[:, :HB, at] = acc[:half].reshape(TM, HB, WIDE)
            kv[:, HB + TB :, at] = acc[half:].reshape(TM, HB, WIDE)

    def attend_space(f, part):
        @pl.loop(part * 4 // GROUP, (part + 1) * 4 // GROUP)
        def _(m):
            places, chains = [], []
            for u in range(GROUP):
                at = pl.ds(pl.multiple_of((m * GROUP + u) * PAIR, PAIR), PAIR)
                vat = pl.ds(pl.multiple_of((m * GROUP + u) * PAIR + D, PAIR), PAIR)
                for h in range(2):
                    rows = slice(h * HB, (h + 1) * HB)
                    keys = slice(h * HB, h * HB + 3 * HB)
                    q = [ref[:, rows, at].reshape(128, PAIR) for ref in (qe, qo)]
                    k = kv[:, keys, at].reshape(384, PAIR)
                    v = kv[:, keys, vat].reshape(384, PAIR)
                    places.append((rows, at))
                    chains.append((jnp.concatenate(q, axis=0), k, v, sbias[f, h]))
            for (rows, at), both in zip(places, attend(chains)):
                ctx[f, :, rows, at] = both.reshape(TM, HB, PAIR)

    back = {}

    def send_context(f):
        for d in range(1, TM):
            t = peer(d)
            cp = rcopy(ctx.at[f, t], cbuf.at[f, me], ts.at[f, d], tr.at[f, d], tm=t)
            cp.start()
            back[f, d] = cp
            pending.append(cp)

    scope = jax.named_scope
    with scope("forward0"):
        forward(0)
    with scope("w1_wait"):
        loads[0].wait()
    with scope("own0"):
        project_own(0)
    with scope("halo0"):
        project_halo(0)
    with scope("attend0"):
        attend_space(0, 0)
    with scope("forward1"):
        forward(1)
    with scope("attend0"):
        attend_space(0, 1)
    with scope("send0"):
        send_context(0)
    with scope("own1"):
        project_own(1)
    with scope("halo1"):
        project_halo(1)
    with scope("attend1"):
        attend_space(1, 0)
        attend_space(1, 1)
    with scope("send1"):
        send_context(1)
        send_cotangent(1)

    loads[1].wait()
    loads[2].wait()
    loads[3].wait()

    def merge(f):
        with scope("wait_ctx"):
            cbuf[f, me] = ctx[f, me]
            for d in range(1, TM):
                back[f, d].wait_recv()

        with scope("merge"):

            @unrolled(D // WIDE)
            def _(n):
                at = slice(n * WIDE, (n + 1) * WIDE)
                acc = jnp.dot(cbuf[f].reshape(TM * TB, D), m1[:, at], preferred_element_type=F32)
                acc = acc + xpos[f, :, :, at].reshape(TM * TB, WIDE).astype(F32)
                mid[f, :, at] = acc.astype(BF16)

            xn2[...] = norm_rows(mid[f], gain2_ref[...])

        with scope("qkv2"):

            @unrolled(D // WIDE)
            def _(n):
                at = slice(n * WIDE, (n + 1) * WIDE)
                acc = jnp.dot(xn2[...], w2[:, at], preferred_element_type=F32)
                qe2[f, :, :, at] = (acc * even_mask).astype(BF16).reshape(TM, TB, WIDE)
                qo2[f, :, :, at] = (acc * odd_mask).astype(BF16).reshape(TM, TB, WIDE)

            @unrolled(2 * D // WIDE)
            def _(n):
                at = slice(n * WIDE, (n + 1) * WIDE)
                wat = slice(n * WIDE + D, (n + 1) * WIDE + D)
                acc = jnp.dot(xn2[...], w2[:, wat], preferred_element_type=F32)
                kv2[f, :, :, at] = acc.astype(BF16).reshape(TM, TB, WIDE)

    def temporal(g):
        places, chains = [], []
        for n in (2 * g, 2 * g + 1):
            at = slice(n * PAIR, (n + 1) * PAIR)
            vat = slice(n * PAIR + D, (n + 1) * PAIR + D)
            for b in range(2):
                rows = slice(b * 16, (b + 1) * 16)
                q = [ref[:, :, rows, at].reshape(256, PAIR) for ref in (qe2, qo2)]
                k = kv2[:, :, rows, at].reshape(256, PAIR)
                v = kv2[:, :, rows, vat].reshape(256, PAIR)
                places.append((rows, at))
                chains.append((jnp.concatenate(q, axis=0), k, v, tbias[...]))
        for (rows, at), both in zip(places, attend(chains)):
            ctx2[:, :, rows, at] = both.reshape(FR, TM, 16, PAIR)

    first = []

    def gradient(g):
        a = ctx2[:, :, :, g * 256 : (g + 1) * 256].reshape(FR * TM * TB, 256)

        @unrolled(D // WIDE)
        def _(n):
            at = slice(n * WIDE, (n + 1) * WIDE)
            c = cot[:, :, :, at].reshape(FR * TM * TB, WIDE)
            acc = lax.dot_general(a, c, (((0,), (0,)), ((), ())), preferred_element_type=F32)
            pbuf[g * 2 : g * 2 + 2, :, :, :, at] = acc.astype(BF16).reshape(2, SP, 2, 16, WIDE)

        cp = rcopy(
            pbuf.at[pl.ds(g * 2, 2), :, 1 - core], ra.at[pl.ds(g * 2, 2)], as_.at[g], ar.at[g], batch=mate
        )
        cp.start()
        pending.append(cp)
        first.append(cp)

    over_z = {}

    def reduce_core(g):
        with scope("reduce_core"):
            first[g].wait_recv()
            rows = pl.ds(g * 2, 2)
            sa[rows] = (pbuf[rows, :, core].astype(F32) + ra[rows].astype(F32)).astype(BF16)
            for d in range(1, SP):
                cp = rcopy(
                    sa.at[rows, zpeer(d)], rb1.at[d - 1, rows], b1s.at[g, d - 1], b1r.at[g, d - 1], space=zpeer(d)
                )
                cp.start()
                over_z[g, d] = cp
                pending.append(cp)

    def reduce_z(g):
        with scope("reduce_z"):
            rows = pl.ds(g * 2, 2)
            total = sa[rows, z].astype(F32)
            for d in range(1, SP):
                over_z[g, d].wait_recv()
                total = total + rb1[d - 1, rows].astype(F32)
            sb1[rows] = total.astype(BF16)

    outs = []

    def output(f):
        @unrolled(D // WIDE)
        def _(n):
            at = slice(n * WIDE, (n + 1) * WIDE)
            acc = jnp.dot(ctx2[f].reshape(TM * TB, D), m2[:, at], preferred_element_type=F32)
            acc = acc + mid[f, :, at].astype(F32)
            obuf[f, :, :, at] = acc.astype(BF16).reshape(TM, TB, WIDE)

    def send_output(f):
        own = pltpu.make_async_copy(obuf.at[f, me], out_hbm.at[f, me], lsem.at[8 + f])
        own.start()
        outs.append(own)
        for d in range(1, TM):
            t = peer(d)
            cp = rcopy(obuf.at[f, t], out_hbm.at[f, me], os_.at[f, d], or_.at[f, d], tm=t)
            cp.start()
            outs.append(cp)

    merge(0)
    merge(1)
    for g in range(4):
        with scope("temporal"):
            temporal(g)
        if g == 1:
            with scope("wait_cot"):
                loads[5].wait()
                for cp in cots:
                    cp.wait_recv()
            with scope("gradient"):
                gradient(0)
        if g > 0:
            with scope("gradient"):
                gradient(g)
        if g > 1:
            reduce_core(g - 2)
    loads[4].wait()
    with scope("output0"):
        output(0)
        send_output(0)
    reduce_core(2)
    with scope("output1"):
        output(1)
        send_output(1)
    reduce_core(3)

    last = []
    for g in range(4):
        reduce_z(g)
    with scope("reduce_tm"):
        for d in range(1, TM):
            t = peer(d)
            cp = rcopy(sb1.at[t], rb2.at[d - 1], b2s.at[d], b2r.at[d], tm=t)
            cp.start()
            last.append(cp)
            pending.append(cp)
        total = sb1[me].astype(F32)
        for d in range(1, TM):
            last[d - 1].wait_recv()
            total = total + rb2[d - 1].astype(F32)
        sb2[...] = total.astype(BF16)
    with scope("reduce_batch"):
        final = []
        for i, other in enumerate(others):
            cp = rcopy(sb2, rb3.at[i], b3s.at[i], b3r.at[i], batch=other)
            cp.start()
            final.append(cp)
        for cp in final:
            cp.wait()
        wg_ref[core] = sb2[...].astype(F32) + rb3[0].astype(F32)
        wg_ref[1 - core] = rb3[1].astype(F32) + rb3[2].astype(F32)

    with scope("wait_out"):
        for cp in pending:
            cp.wait_send()
        for cp in outs:
            cp.wait()


def per_device(
    clip_tokens,
    frame_order,
    row_reach,
    spatial_gain,
    spatial_heads,
    spatial_merge,
    temporal_gain,
    temporal_heads,
    temporal_merge,
    cotangent,
):
    tokens = clip_tokens.reshape(TM, FR, TB, D).transpose(1, 0, 2, 3)
    grads = cotangent.reshape(FR, 8, TM, 4, D).transpose(2, 0, 1, 3, 4).reshape(TM, FR, TB, D)
    dma = pltpu.SemaphoreType.DMA
    vm = pltpu.VMEM
    smem = pl.BlockSpec(memory_space=pltpu.SMEM)
    vmem = pl.BlockSpec(memory_space=pltpu.VMEM)
    anym = pl.BlockSpec(memory_space=pl.ANY)
    out, wg = pl.pallas_call(
        kernel,
        out_shape=[
            jax.ShapeDtypeStruct((FR, TM, TB, D), BF16),
            jax.ShapeDtypeStruct((2, 16, D), F32),
        ],
        in_specs=[smem, smem, vmem, vmem] + [anym] * 6,
        out_specs=[anym, vmem],
        scratch_shapes=[
            vm((D, 3 * D), BF16),
            vm((D, D), BF16),
            vm((D, 3 * D), BF16),
            vm((D, D), BF16),
            vm((FR, TM, EXT, D), BF16),
            vm((TM * TB, D), BF16),
            vm((TM, TB, D), BF16),
            vm((TM, TB, D), BF16),
            vm((TM, EXT, 2 * D), BF16),
            vm((FR, 2, 384, 256), F32),
            vm((FR, TM, TB, D), BF16),
            vm((FR, TM, TB, D), BF16),
            vm((FR, TM, TB, D), BF16),
            vm((FR, TM * TB, D), BF16),
            vm((TM * TB, D), BF16),
            vm((FR, TM, TB, D), BF16),
            vm((FR, TM, TB, D), BF16),
            vm((FR, TM, TB, 2 * D), BF16),
            vm((256, 512), F32),
            vm((FR, TM, TB, D), BF16),
            vm((FR, TM, TB, D), BF16),
            vm((FR, TM, TB, D), BF16),
            vm((TM, SP, 2, 16, D), BF16),
            vm((TM, SP, 16, D), BF16),
            vm((TM, SP, 16, D), BF16),
            vm((SP - 1, TM, 16, D), BF16),
            vm((TM, 16, D), BF16),
            vm((TM - 1, 16, D), BF16),
            vm((16, D), BF16),
            vm((3, 16, D), BF16),
            dma((10,)),
            dma((FR, TM)),
            dma((FR, TM)),
            dma((FR, TM, 2)),
            dma((FR, TM, 2)),
            dma((FR, TM)),
            dma((FR, TM)),
            dma((FR, TM)),
            dma((FR, TM)),
            dma((FR, TM)),
            dma((FR, TM)),
            dma((4,)),
            dma((4,)),
            dma((4, SP - 1)),
            dma((4, SP - 1)),
            dma((TM,)),
            dma((TM,)),
            dma((3,)),
            dma((3,)),
        ],
        compiler_params=pltpu.CompilerParams(
            collective_id=0, has_side_effects=True, vmem_limit_bytes=62 * 1024 * 1024
        ),
    )(
        frame_order,
        row_reach,
        spatial_gain.reshape(1, D),
        temporal_gain.reshape(1, D),
        tokens,
        grads,
        spatial_heads,
        spatial_merge,
        temporal_heads,
        temporal_merge,
    )
    out = out.reshape(FR, TM, 8, 4, D).transpose(0, 2, 1, 3, 4).reshape(1, FR, 8, 32, D)
    return out, wg.reshape(32, D)


def solution(mesh):
    in_specs = (
        P("batch", None, "space", "tm", None),
        P("batch", None),
        P("batch", "tm"),
        P(),
        P(),
        P(),
        P(),
        P(),
        P(),
        P("batch", "tm", "space", None, None),
    )
    out_specs = (P("batch", "tm", "space", None, None), P(("tm", "space"), None))
    return jax.shard_map(
        per_device, mesh=mesh, in_specs=in_specs, out_specs=out_specs, check_vma=False
    )
```

```python
import functools
import math

import jax
import jax.numpy as jnp
from jax import lax
from jax.experimental import pallas as pl
from jax.experimental.pallas import tpu as pltpu
from jax.sharding import PartitionSpec as P

D = 1024
HEAD_DIM = 64
FLOOR = 0.5
TM = 8
SP = 4
FR = 2
TB = 32
HB = 16
EXT = TB + 2 * HB
PAIR = 128
WIDE = 1024
GROUP = 2
NEG = -1e30
QSCALE = HEAD_DIM**-0.5 * math.log2(math.e)
MESH = pl.DeviceIdType.MESH
F32 = jnp.float32
BF16 = jnp.bfloat16


def exchange_halves(a, b):
    first = iota((1, 8, 1), 1) < 4
    return jnp.where(first, a, pltpu.roll(b, 4, 1)), jnp.where(first, pltpu.roll(a, 4, 1), b)


def unrolled(count):
    def run(body):
        for n in range(count):
            body(n)

    return run


def norm_rows(values, gain):
    x = values.astype(F32).reshape(-1, D)
    x = x * lax.rsqrt(jnp.mean(x * x, axis=-1, keepdims=True) + FLOOR)
    return (x * gain).astype(BF16)


def head_masks(width):
    lane = lax.broadcasted_iota(jnp.int32, (1, width), 1)
    odd = lax.rem(lane // HEAD_DIM, 2).astype(F32)
    return (1.0 - odd) * QSCALE, odd * QSCALE


def iota(shape, dim):
    return lax.broadcasted_iota(jnp.int32, shape, dim)


def attend(chains):
    scores = [
        lax.dot_general(k, q, (((1,), (1,)), ((), ())), preferred_element_type=F32) + bias
        for q, k, _, bias in chains
    ]
    weights = []
    for s in scores:
        p = jnp.exp2(s - jnp.max(s, axis=0, keepdims=True))
        weights.append((p.astype(BF16), 1.0 / jnp.sum(p, axis=0, keepdims=True)))
    outputs = []
    for (q, _, v, _), (p, scale) in zip(chains, weights):
        count = q.shape[0] // 2
        o = lax.dot_general(v, p, (((0,), (0,)), ((), ())), preferred_element_type=F32) * scale
        both = jnp.where(iota((PAIR, count), 0) < HEAD_DIM, o[:, :count], o[:, count:])
        outputs.append(both.T.astype(BF16))
    return outputs


def kernel(
    order_ref,
    reach_ref,
    gain1_ref,
    gain2_ref,
    x_hbm,
    cot_hbm,
    w1_hbm,
    m1_hbm,
    w2_hbm,
    m2_hbm,
    out_hbm,
    wg_ref,
    w1,
    m1,
    w2,
    m2,
    xbuf,
    xn,
    qe,
    qo,
    kv,
    sbias,
    ctx,
    cbuf,
    xpos,
    mid,
    xn2,
    qe2,
    qo2,
    kv2,
    tbias,
    ctx2,
    cotraw,
    cot,
    cotin,
    obuf,
    pbuf,
    ra,
    sa,
    rb1,
    sb1,
    rb2,
    sb2,
    rb3,
    lsem,
    xs,
    xr,
    hs,
    hr,
    ts,
    tr,
    cs,
    cr,
    os_,
    or_,
    as_,
    ar,
    b1s,
    b1r,
    b2s,
    b2r,
    b3s,
    b3r,
):
    me = lax.axis_index("tm")
    z = lax.axis_index("space")
    batch = lax.axis_index("batch")
    core = lax.rem(batch, 2)
    mate = batch + 1 - 2 * core
    others = (lax.rem(batch + 2, 4), mate, lax.rem(mate + 2, 4))

    steps = ((0, 0), (0, 1), (1, 0), (3, 0), (1, 1), (3, 1), (2, 0), (2, 1))

    def peer(d, sign=1):
        dx, dy = steps[d]
        x = lax.rem(me // 2 + 4 + sign * dx, 4)
        return x * 2 + lax.rem(lax.rem(me, 2) + dy, 2)

    def zpeer(d):
        return lax.rem(z + d, SP)

    def rcopy(src, dst, send, recv, **where):
        return pltpu.make_async_remote_copy(
            src_ref=src, dst_ref=dst, send_sem=send, recv_sem=recv, device_id=where, device_id_type=MESH
        )

    def took(ref, sem):
        pltpu.make_async_copy(ref, ref, sem).wait()

    loads = [
        pltpu.make_async_copy(w1_hbm, w1, lsem.at[0]),
        pltpu.make_async_copy(x_hbm, xpos, lsem.at[1]),
        pltpu.make_async_copy(m1_hbm, m1, lsem.at[2]),
        pltpu.make_async_copy(w2_hbm, w2, lsem.at[3]),
        pltpu.make_async_copy(m2_hbm, m2, lsem.at[4]),
        pltpu.make_async_copy(cot_hbm, cotraw, lsem.at[5]),
        pltpu.make_async_copy(x_hbm.at[me, 0], xbuf.at[0, me, pl.ds(4, 8)], lsem.at[6]),
        pltpu.make_async_copy(x_hbm.at[me, 1], xbuf.at[1, me, pl.ds(4, 8)], lsem.at[7]),
    ]
    for i in (6, 7, 0, 5, 1, 2, 3, 4):
        loads[i].start()

    barrier = pltpu.get_barrier_semaphore()
    for d in range(1, TM):
        pl.semaphore_signal(barrier, inc=1, device_id={"tm": peer(d)}, device_id_type=MESH)
    for d in range(1, SP):
        pl.semaphore_signal(barrier, inc=1, device_id={"space": zpeer(d)}, device_id_type=MESH)
    for other in others:
        pl.semaphore_signal(barrier, inc=1, device_id={"batch": other}, device_id_type=MESH)
    with jax.named_scope("barrier"):
        pl.semaphore_wait(barrier, TM - 1 + SP - 1 + 3)

    sent = []

    tok = {}
    for f in range(FR):
        for d in range(1, TM):
            t = peer(d)
            tok[f, d] = rcopy(x_hbm.at[t, f], xbuf.at[f, me, pl.ds(4, 8)], xs.at[f], xr.at[f, d], tm=t)
            if f == 0:
                tok[f, d].start()
    tokens_sent = xpos.at[pl.ds(0, TM - 1), 0]

    def send_cotangent(f):
        for d in range(1, TM):
            t = peer(d)
            rcopy(cot.at[f, t], cotin.at[f, me], cs.at[f], cr.at[f], tm=t).start()
        sent.append((cot.at[f, pl.ds(0, TM - 1)], cs.at[f]))

    order_key = jnp.zeros((256, 1), jnp.int32)
    order_query = jnp.zeros((1, 512), jnp.int32)
    key_slot = iota((256, 1), 0) // 16
    query_slot = lax.rem(iota((1, 512), 1) // 16, 16)
    for f in range(FR):
        for s in range(TM):
            value = order_ref[0, s * FR + f]
            order_key = jnp.where(key_slot == f * TM + s, value, order_key)
            order_query = jnp.where(query_slot == f * TM + s, value, order_query)
    same = lax.rem(iota((256, 512), 0), 16) == lax.rem(iota((256, 512), 1), 16)
    tbias[...] = jnp.where(same & (order_key <= order_query), 0.0, NEG)
    key = iota((384, 1), 0)
    key_src = jnp.zeros((384, 1), jnp.int32)
    for n in range(1, TM):
        key_src = key_src + (key >= 48 * n).astype(jnp.int32)
    key_row = (key - 48 * key_src) // 4 - 4
    query_row = lax.rem(iota((1, 256), 1), 16) // 4
    distance = jnp.abs(key_row - query_row)
    for f in range(FR):
        for h in range(2):
            row = key_row + (z * 8 + 4 * h)
            keep = (distance <= reach_ref[0, f]) & (row >= 0) & (row < 8 * SP)
            sbias[f, h] = jnp.where(keep, 0.0, NEG)

    loads[5].wait()
    with jax.named_scope("shuffle"):
        for f in range(FR):
            for j in range(TM // 2):
                c = cotraw[f, :, 8 * j : 8 * j + 8].astype(F32).reshape(4, 2, 8, D)
                for i, block in enumerate(exchange_halves(c[:, 0], c[:, 1])):
                    cot[f, 2 * j + i] = block.reshape(TB, D).astype(BF16)
    even_mask, odd_mask = head_masks(WIDE)


    def forward(f):
        for d in range(TM):
            if d == 0:
                loads[6 + f].wait()
            else:
                if f == 0 and d == TM - 3:
                    took(tokens_sent, xs.at[0])
                    for n in range(1, TM):
                        tok[1, n].start()
                tok[f, d].wait_recv()
            s = peer(d, -1)
            above, below = zpeer(SP - 1), zpeer(1)
            rcopy(xbuf.at[f, s, pl.ds(4, 4)], xbuf.at[f, s, pl.ds(12, 4)], hs.at[f], hr.at[f], space=above).start()
            rcopy(xbuf.at[f, s, pl.ds(8, 4)], xbuf.at[f, s, pl.ds(0, 4)], hs.at[f], hr.at[f], space=below).start()
        sent.append((xbuf.at[f, :, pl.ds(4, 8)], hs.at[f]))

    def project_own(f):
        xn[...] = norm_rows(xbuf[f, :, 4:12], gain1_ref[...])

        @unrolled(D // WIDE)
        def _(n):
            at = slice(n * WIDE, (n + 1) * WIDE)
            acc = jnp.dot(xn[...], w1[:, at], preferred_element_type=F32)
            qe[:, :, at] = (acc * even_mask).astype(BF16).reshape(TM, TB, WIDE)
            qo[:, :, at] = (acc * odd_mask).astype(BF16).reshape(TM, TB, WIDE)

        @unrolled(2 * D // WIDE)
        def _(n):
            at = slice(n * WIDE, (n + 1) * WIDE)
            wat = slice(n * WIDE + D, (n + 1) * WIDE + D)
            acc = jnp.dot(xn[...], w1[:, wat], preferred_element_type=F32)
            kv[:, HB : HB + TB, at] = acc.astype(BF16).reshape(TM, TB, WIDE)

    def project_halo(f):
        took(xbuf.at[f, :, pl.ds(4, 8)], hr.at[f])
        half = TM * HB
        xn[:half] = norm_rows(xbuf[f, :, :4], gain1_ref[...])
        xn[half:] = norm_rows(xbuf[f, :, 12:], gain1_ref[...])

        @unrolled(2 * D // WIDE)
        def _(n):
            at = slice(n * WIDE, (n + 1) * WIDE)
            wat = slice(n * WIDE + D, (n + 1) * WIDE + D)
            acc = jnp.dot(xn[...], w1[:, wat], preferred_element_type=F32).astype(BF16)
            kv[:, :HB, at] = acc[:half].reshape(TM, HB, WIDE)
            kv[:, HB + TB :, at] = acc[half:].reshape(TM, HB, WIDE)

    def attend_space(f, part):
        @pl.loop(0, 4 // GROUP)
        def _(m):
            places, chains = [], []
            for u in range(GROUP):
                first_col = (m * GROUP + u) * PAIR
                to = pl.ds(pl.multiple_of(first_col, PAIR), PAIR)
                at = pl.ds(pl.multiple_of(first_col + part * 512, PAIR), PAIR)
                vat = pl.ds(pl.multiple_of(first_col + part * 512 + D, PAIR), PAIR)
                for h in range(2):
                    rows = slice(h * HB, (h + 1) * HB)
                    keys = slice(h * HB, h * HB + 3 * HB)
                    q = [ref[:, rows, at].reshape(128, PAIR) for ref in (qe, qo)]
                    k = kv[:, keys, at].reshape(384, PAIR)
                    v = kv[:, keys, vat].reshape(384, PAIR)
                    places.append((rows, to))
                    chains.append((jnp.concatenate(q, axis=0), k, v, sbias[f, h]))
            for (rows, to), both in zip(places, attend(chains)):
                ctx[f, part, :, rows, to] = both.reshape(TM, HB, PAIR)

    def send_context(f, part):
        cbuf[f, part, me] = ctx[f, part, me]
        for d in range(1, TM):
            t = peer(d)
            rcopy(ctx.at[f, part, t], cbuf.at[f, part, me], ts.at[f, part], tr.at[f, part], tm=t).start()
        if f == 0:
            sent.append((ctx.at[f, part, pl.ds(0, TM - 1)], ts.at[f, part]))

    scope = jax.named_scope
    with scope("forward0"):
        forward(0)
    send_cotangent(0)
    with scope("w1_wait"):
        loads[0].wait()
    with scope("own0"):
        project_own(0)
    with scope("halo0"):
        project_halo(0)
    with scope("attend0"):
        attend_space(0, 0)
        send_context(0, 0)
    with scope("forward1"):
        forward(1)
    with scope("attend0"):
        attend_space(0, 1)
        send_context(0, 1)
    with scope("own1"):
        project_own(1)
    with scope("halo1"):
        project_halo(1)
    with scope("attend1"):
        attend_space(1, 0)
        send_context(1, 0)
        attend_space(1, 1)
        send_context(1, 1)

    loads[1].wait()
    loads[2].wait()
    loads[3].wait()

    def merged(parts, tokens):
        joined = jnp.concatenate([parts[0], parts[1]], axis=-1).reshape(TM * TB, D)
        acc = jnp.dot(joined, m1[...], preferred_element_type=F32)
        return (acc + tokens.astype(F32).reshape(TM * TB, D)).astype(BF16)

    def merge(f):
        with scope("wait_ctx"):
            if f == 1:
                for part in range(2):
                    took(ctx.at[f, part, pl.ds(0, TM - 1)], ts.at[f, part])
                send_cotangent(1)
            for part in range(2):
                took(cbuf.at[f, part, pl.ds(0, TM - 1)], tr.at[f, part])

        with scope("merge"):
            mid[f] = merged((cbuf[f, 0], cbuf[f, 1]), xpos[:, f])
            xn2[...] = norm_rows(mid[f], gain2_ref[...])

        with scope("qkv2"):

            @unrolled(D // WIDE)
            def _(n):
                at = slice(n * WIDE, (n + 1) * WIDE)
                acc = jnp.dot(xn2[...], w2[:, at], preferred_element_type=F32)
                qe2[f, :, :, at] = (acc * even_mask).astype(BF16).reshape(TM, TB, WIDE)
                qo2[f, :, :, at] = (acc * odd_mask).astype(BF16).reshape(TM, TB, WIDE)

            @unrolled(2 * D // WIDE)
            def _(n):
                at = slice(n * WIDE, (n + 1) * WIDE)
                wat = slice(n * WIDE + D, (n + 1) * WIDE + D)
                acc = jnp.dot(xn2[...], w2[:, wat], preferred_element_type=F32)
                kv2[f, :, :, at] = acc.astype(BF16).reshape(TM, TB, WIDE)

    def temporal(g):
        places, chains = [], []
        for n in (2 * g, 2 * g + 1):
            at = slice(n * PAIR, (n + 1) * PAIR)
            vat = slice(n * PAIR + D, (n + 1) * PAIR + D)
            for b in range(2):
                rows = slice(b * 16, (b + 1) * 16)
                q = [ref[:, :, rows, at].reshape(256, PAIR) for ref in (qe2, qo2)]
                k = kv2[:, :, rows, at].reshape(256, PAIR)
                v = kv2[:, :, rows, vat].reshape(256, PAIR)
                places.append((rows, slice(n % 2 * PAIR, (n % 2 + 1) * PAIR)))
                chains.append((jnp.concatenate(q, axis=0), k, v, tbias[...]))
        for (rows, at), both in zip(places, attend(chains)):
            ctx2[g, :, :, rows, at] = both.reshape(FR, TM, 16, PAIR)

    first = []

    def gradient(g):
        a = ctx2[g].reshape(FR * TM * TB, 256)

        @unrolled(D // WIDE)
        def _(n):
            at = slice(n * WIDE, (n + 1) * WIDE)
            c = cotin[:, :, :, at].reshape(FR * TM * TB, WIDE)
            acc = lax.dot_general(a, c, (((0,), (0,)), ((), ())), preferred_element_type=F32)
            pbuf[g * 2 : g * 2 + 2, :, :, :, at] = acc.astype(BF16).reshape(2, SP, 2, 16, WIDE)

        cp = rcopy(
            pbuf.at[pl.ds(g * 2, 2), :, 1 - core], ra.at[pl.ds(g * 2, 2)], as_.at[g], ar.at[g], batch=mate
        )
        cp.start()
        first.append(cp)

    def reduce_core(g):
        with scope("reduce_core"):
            first[g].wait()
            rows = pl.ds(g * 2, 2)
            sa[rows] = (pbuf[rows, :, core].astype(F32) + ra[rows].astype(F32)).astype(BF16)
            for d in range(1, SP):
                rcopy(sa.at[rows, zpeer(d)], rb1.at[d - 1, rows], b1s.at[g], b1r.at[g], space=zpeer(d)).start()
            sent.append((sa.at[rows, pl.ds(0, SP - 1)], b1s.at[g]))

    def reduce_z(g):
        with scope("reduce_z"):
            rows = pl.ds(g * 2, 2)
            took(rb1.at[:, rows], b1r.at[g])
            total = sa[rows, z].astype(F32)
            for d in range(1, SP):
                total = total + rb1[d - 1, rows].astype(F32)
            sb1[rows] = total.astype(BF16)

    outs = []

    def output(f):
        joined = jnp.concatenate([ctx2[g, f].reshape(TM * TB, 256) for g in range(4)], axis=-1)
        acc = jnp.dot(joined, m2[...], preferred_element_type=F32) + mid[f].astype(F32)
        obuf[f] = acc.astype(BF16).reshape(TM, TB, D)
        cp = pltpu.make_async_copy(obuf.at[f, me], out_hbm.at[f, me], lsem.at[8 + f])
        cp.start()
        outs.append(cp)
        for d in range(1, TM):
            t = peer(d)
            rcopy(obuf.at[f, t], out_hbm.at[f, me], os_.at[f], or_.at[f], tm=t).start()
        sent.append((obuf.at[f, pl.ds(0, TM - 1)], os_.at[f]))
        sent.append((obuf.at[f, pl.ds(0, TM - 1)], or_.at[f]))

    merge(0)
    merge(1)
    with scope("temporal"):
        temporal(0)
        temporal(1)
    loads[4].wait()
    with scope("wait_cot"):
        for f in range(FR):
            cotin[f, me] = cot[f, me]
            took(cotin.at[f, pl.ds(0, TM - 1)], cr.at[f])
    with scope("gradient"):
        gradient(0)
        gradient(1)
    reduce_core(0)
    for g in (2, 3):
        with scope("temporal"):
            temporal(g)
        with scope("gradient"):
            gradient(g)
        reduce_core(g - 1)
    with scope("output0"):
        output(0)
    reduce_core(3)
    with scope("output1"):
        output(1)

    for g in range(4):
        reduce_z(g)
    with scope("reduce_tm"):
        for d in range(1, TM):
            t = peer(d)
            rcopy(sb1.at[t], rb2.at[d - 1], b2s, b2r, tm=t).start()
        sent.append((sb1.at[pl.ds(0, TM - 1)], b2s))
        took(rb2, b2r)
        total = sb1[me].astype(F32)
        for d in range(1, TM):
            total = total + rb2[d - 1].astype(F32)
        sb2[...] = total.astype(BF16)
    with scope("reduce_batch"):
        for i, other in enumerate(others):
            rcopy(sb2, rb3.at[i], b3s, b3r, batch=other).start()
        took(rb3, b3r)
        wg_ref[core] = sb2[...].astype(F32) + rb3[0].astype(F32)
        wg_ref[1 - core] = rb3[1].astype(F32) + rb3[2].astype(F32)

    with scope("wait_out"):
        took(rb3, b3s)
        took(tokens_sent, xs.at[1])
        for ref, sem in sent:
            took(ref, sem)
        for cp in outs:
            cp.wait()


def arrange(blocks_ref, grad_ref, out_ref, wg_ref):
    halves = []
    for j in range(2):
        a = blocks_ref[0, 2 * j].astype(F32).reshape(4, 8, D)
        b = blocks_ref[0, 2 * j + 1].astype(F32).reshape(4, 8, D)
        halves.append(exchange_halves(a, b))
    for i in range(2):
        rows = jnp.concatenate([halves[0][i], halves[1][i]], axis=1).astype(BF16)
        for r in range(4):
            out_ref[0, 2 * r + i] = rows[r]
    wg_ref[...] = grad_ref[...]


def per_device(
    clip_tokens,
    frame_order,
    row_reach,
    spatial_gain,
    spatial_heads,
    spatial_merge,
    temporal_gain,
    temporal_heads,
    temporal_merge,
    cotangent,
):
    tokens = clip_tokens.reshape(TM, FR, 8, 4, D)
    grads = cotangent.reshape(FR, 8, 32, D)
    dma = pltpu.SemaphoreType.DMA
    vm = pltpu.VMEM
    smem = pl.BlockSpec(memory_space=pltpu.SMEM)
    vmem = pl.BlockSpec(memory_space=pltpu.VMEM)
    anym = pl.BlockSpec(memory_space=pl.ANY)
    blocks, grad = pl.pallas_call(
        kernel,
        out_shape=[
            jax.ShapeDtypeStruct((FR, TM, TB, D), BF16),
            jax.ShapeDtypeStruct((2, 16, D), F32),
        ],
        in_specs=[smem, smem, vmem, vmem] + [anym] * 6,
        out_specs=[anym, vmem],
        scratch_shapes=[
            vm((D, 3 * D), BF16),
            vm((D, D), BF16),
            vm((D, 3 * D), BF16),
            vm((D, D), BF16),
            vm((FR, TM, 16, 4, D), BF16),
            vm((TM * TB, D), BF16),
            vm((TM, TB, D), BF16),
            vm((TM, TB, D), BF16),
            vm((TM, EXT, 2 * D), BF16),
            vm((FR, 2, 384, 256), F32),
            vm((FR, 2, TM, TB, 512), BF16),
            vm((FR, 2, TM, TB, 512), BF16),
            vm((TM, FR, 8, 4, D), BF16),
            vm((FR, TM * TB, D), BF16),
            vm((TM * TB, D), BF16),
            vm((FR, TM, TB, D), BF16),
            vm((FR, TM, TB, D), BF16),
            vm((FR, TM, TB, 2 * D), BF16),
            vm((256, 512), F32),
            vm((4, FR, TM, TB, 256), BF16),
            vm((FR, 8, 32, D), BF16),
            vm((FR, TM, TB, D), BF16),
            vm((FR, TM, TB, D), BF16),
            vm((FR, TM, TB, D), BF16),
            vm((TM, SP, 2, 16, D), BF16),
            vm((TM, SP, 16, D), BF16),
            vm((TM, SP, 16, D), BF16),
            vm((SP - 1, TM, 16, D), BF16),
            vm((TM, 16, D), BF16),
            vm((TM - 1, 16, D), BF16),
            vm((16, D), BF16),
            vm((3, 16, D), BF16),
            dma((10,)),
            dma((FR,)),
            dma((FR, TM)),
            dma((FR,)),
            dma((FR,)),
            dma((FR, 2)),
            dma((FR, 2)),
            dma((FR,)),
            dma((FR,)),
            dma((FR,)),
            dma((FR,)),
            dma((4,)),
            dma((4,)),
            dma((4,)),
            dma((4,)),
            dma,
            dma,
            dma,
            dma,
        ],
        compiler_params=pltpu.CompilerParams(
            collective_id=0, has_side_effects=True, vmem_limit_bytes=62 * 1024 * 1024
        ),
    )(
        frame_order,
        row_reach,
        spatial_gain.reshape(1, D),
        temporal_gain.reshape(1, D),
        tokens,
        grads,
        spatial_heads,
        spatial_merge,
        temporal_heads,
        temporal_merge,
    )
    out, wg = pl.pallas_call(
        arrange,
        grid=(FR, 2),
        out_shape=[
            jax.ShapeDtypeStruct((FR, 8, 32, D), BF16),
            jax.ShapeDtypeStruct((2, 16, D), F32),
        ],
        in_specs=[
            pl.BlockSpec((1, 4, TB, D), lambda f, k: (f, k, 0, 0)),
            pl.BlockSpec((2, 16, D), lambda f, k: (0, 0, 0)),
        ],
        out_specs=[
            pl.BlockSpec((1, 8, 16, D), lambda f, k: (f, 0, k, 0)),
            pl.BlockSpec((2, 16, D), lambda f, k: (0, 0, 0)),
        ],
    )(blocks, grad)
    return out.reshape(1, FR, 8, 32, D), wg.reshape(32, D)


def solution(mesh):
    in_specs = (
        P("batch", None, "space", "tm", None),
        P("batch", None),
        P("batch", "tm"),
        P(),
        P(),
        P(),
        P(),
        P(),
        P(),
        P("batch", "tm", "space", None, None),
    )
    out_specs = (P("batch", "tm", "space", None, None), P(("tm", "space"), None))
    return jax.shard_map(
        per_device, mesh=mesh, in_specs=in_specs, out_specs=out_specs, check_vma=False
    )
```

```python
import functools
import math

import jax
import jax.numpy as jnp
from jax import lax
from jax.experimental import pallas as pl
from jax.experimental.pallas import tpu as pltpu
from jax.sharding import PartitionSpec as P

D = 1024
HEAD_DIM = 64
FLOOR = 0.5
TM = 8
SP = 4
FR = 2
TB = 32
HB = 16
EXT = TB + 2 * HB
PAIR = 128
WIDE = 1024
GROUP = 2
NEG = -1e30
QSCALE = HEAD_DIM**-0.5 * math.log2(math.e)
MESH = pl.DeviceIdType.MESH
F32 = jnp.float32
BF16 = jnp.bfloat16


def exchange_halves(a, b):
    first = iota((1, 8, 1), 1) < 4
    return jnp.where(first, a, pltpu.roll(b, 4, 1)), jnp.where(first, pltpu.roll(a, 4, 1), b)


def unrolled(count):
    def run(body):
        for n in range(count):
            body(n)

    return run


def norm_rows(values, gain):
    x = values.astype(F32).reshape(-1, D)
    x = x * lax.rsqrt(jnp.mean(x * x, axis=-1, keepdims=True) + FLOOR)
    return (x * gain).astype(BF16)


def head_masks(width):
    lane = lax.broadcasted_iota(jnp.int32, (1, width), 1)
    odd = lax.rem(lane // HEAD_DIM, 2).astype(F32)
    return (1.0 - odd) * QSCALE, odd * QSCALE


def iota(shape, dim):
    return lax.broadcasted_iota(jnp.int32, shape, dim)


def attend(chains):
    scores = [
        lax.dot_general(k, q, (((1,), (1,)), ((), ())), preferred_element_type=F32) + bias
        for q, k, _, bias in chains
    ]
    weights = []
    for s in scores:
        p = jnp.exp2(s - jnp.max(s, axis=0, keepdims=True))
        weights.append((p.astype(BF16), 1.0 / jnp.sum(p, axis=0, keepdims=True)))
    outputs = []
    for (q, _, v, _), (p, scale) in zip(chains, weights):
        count = q.shape[0] // 2
        o = lax.dot_general(v, p, (((0,), (0,)), ((), ())), preferred_element_type=F32) * scale
        both = jnp.where(iota((PAIR, count), 0) < HEAD_DIM, o[:, :count], o[:, count:])
        outputs.append(both.T.astype(BF16))
    return outputs


def kernel(
    order_ref,
    reach_ref,
    gain1_ref,
    gain2_ref,
    x_hbm,
    cot_hbm,
    w1_hbm,
    m1_hbm,
    w2_hbm,
    m2_hbm,
    out_hbm,
    wg_ref,
    w1,
    m1,
    w2,
    m2,
    xbuf,
    xn,
    qe,
    qo,
    kv,
    sbias,
    ctx,
    cbuf,
    xpos,
    mid,
    xn2,
    qe2,
    qo2,
    kv2,
    tbias,
    ctx2,
    cotraw,
    cot,
    cotin,
    obuf,
    pbuf,
    ra,
    sa,
    rb1,
    sb1,
    rb2,
    sb2,
    rb3,
    lsem,
    xs,
    xr,
    hs,
    hr,
    ts,
    tr,
    cs,
    cr,
    os_,
    or_,
    as_,
    ar,
    b1s,
    b1r,
    b2s,
    b2r,
    b3s,
    b3r,
):
    me = lax.axis_index("tm")
    z = lax.axis_index("space")
    batch = lax.axis_index("batch")
    core = lax.rem(batch, 2)
    mate = batch + 1 - 2 * core
    others = (lax.rem(batch + 2, 4), mate, lax.rem(mate + 2, 4))

    steps = ((0, 0), (0, 1), (1, 0), (3, 0), (1, 1), (3, 1), (2, 0), (2, 1))

    def peer(d, sign=1):
        dx, dy = steps[d]
        x = lax.rem(me // 2 + 4 + sign * dx, 4)
        return x * 2 + lax.rem(lax.rem(me, 2) + dy, 2)

    def zpeer(d):
        return lax.rem(z + d, SP)

    def rcopy(src, dst, send, recv, **where):
        return pltpu.make_async_remote_copy(
            src_ref=src, dst_ref=dst, send_sem=send, recv_sem=recv, device_id=where, device_id_type=MESH
        )

    def took(ref, sem):
        pltpu.make_async_copy(ref, ref, sem).wait()

    loads = [
        pltpu.make_async_copy(w1_hbm, w1, lsem.at[0]),
        pltpu.make_async_copy(x_hbm, xpos, lsem.at[1]),
        pltpu.make_async_copy(m1_hbm, m1, lsem.at[2]),
        pltpu.make_async_copy(w2_hbm, w2, lsem.at[3]),
        pltpu.make_async_copy(m2_hbm, m2, lsem.at[4]),
        pltpu.make_async_copy(cot_hbm, cotraw, lsem.at[5]),
        pltpu.make_async_copy(x_hbm.at[me, 0], xbuf.at[0, me, pl.ds(4, 8)], lsem.at[6]),
        pltpu.make_async_copy(x_hbm.at[me, 1], xbuf.at[1, me, pl.ds(4, 8)], lsem.at[7]),
    ]
    for i in (6, 7, 0, 5, 1, 2, 3, 4):
        loads[i].start()

    barrier = pltpu.get_barrier_semaphore()
    for d in range(1, TM):
        pl.semaphore_signal(barrier, inc=1, device_id={"tm": peer(d)}, device_id_type=MESH)
    for d in range(1, SP):
        pl.semaphore_signal(barrier, inc=1, device_id={"space": zpeer(d)}, device_id_type=MESH)
    for other in others:
        pl.semaphore_signal(barrier, inc=1, device_id={"batch": other}, device_id_type=MESH)
    with jax.named_scope("barrier"):
        pl.semaphore_wait(barrier, TM - 1 + SP - 1 + 3)

    sent = []

    tok = {}
    for f in range(FR):
        for d in range(1, TM):
            t = peer(d)
            tok[f, d] = rcopy(x_hbm.at[t, f], xbuf.at[f, me, pl.ds(4, 8)], xs.at[f], xr.at[f, d], tm=t)
            if f == 0:
                tok[f, d].start()
    tokens_sent = xpos.at[pl.ds(0, TM - 1), 0]

    def send_cotangent(f):
        for d in range(1, TM):
            t = peer(d)
            rcopy(cot.at[f, t], cotin.at[f, me], cs.at[f], cr.at[f], tm=t).start()
        sent.append((cot.at[f, pl.ds(0, TM - 1)], cs.at[f]))

    order_key = jnp.zeros((256, 1), jnp.int32)
    order_query = jnp.zeros((1, 512), jnp.int32)
    key_slot = iota((256, 1), 0) // 16
    query_slot = lax.rem(iota((1, 512), 1) // 16, 16)
    for f in range(FR):
        for s in range(TM):
            value = order_ref[0, s * FR + f]
            order_key = jnp.where(key_slot == f * TM + s, value, order_key)
            order_query = jnp.where(query_slot == f * TM + s, value, order_query)
    same = lax.rem(iota((256, 512), 0), 16) == lax.rem(iota((256, 512), 1), 16)
    tbias[...] = jnp.where(same & (order_key <= order_query), 0.0, NEG)
    key = iota((384, 1), 0)
    key_src = jnp.zeros((384, 1), jnp.int32)
    for n in range(1, TM):
        key_src = key_src + (key >= 48 * n).astype(jnp.int32)
    key_row = (key - 48 * key_src) // 4 - 4
    query_row = lax.rem(iota((1, 256), 1), 16) // 4
    distance = jnp.abs(key_row - query_row)
    for f in range(FR):
        for h in range(2):
            row = key_row + (z * 8 + 4 * h)
            keep = (distance <= reach_ref[0, f]) & (row >= 0) & (row < 8 * SP)
            sbias[f, h] = jnp.where(keep, 0.0, NEG)

    loads[5].wait()
    with jax.named_scope("shuffle"):
        for f in range(FR):
            for j in range(TM // 2):
                c = cotraw[f, :, 8 * j : 8 * j + 8].astype(F32).reshape(4, 2, 8, D)
                for i, block in enumerate(exchange_halves(c[:, 0], c[:, 1])):
                    cot[f, 2 * j + i] = block.reshape(TB, D).astype(BF16)
    even_mask, odd_mask = head_masks(WIDE)

    has_above, has_below = z > 0, z < SP - 1

    @pl.when(z == 0)
    def _():
        xbuf[:, :, :4] = jnp.zeros((FR, TM, 4, 4, D), BF16)

    @pl.when(z == SP - 1)
    def _():
        xbuf[:, :, 12:] = jnp.zeros((FR, TM, 4, 4, D), BF16)


    def forward(f, slots):
        for d in slots:
            if d == 0:
                loads[6 + f].wait()
            else:
                if f == 0 and d == TM - 3:
                    took(tokens_sent, xs.at[0])
                    for n in range(1, TM):
                        tok[1, n].start()
                tok[f, d].wait_recv()
            s = peer(d, -1)
            own = xbuf.at[f, s]

            @pl.when(has_above)
            def _():
                rcopy(own.at[pl.ds(4, 4)], own.at[pl.ds(12, 4)], hs.at[f, 0], hr.at[f, 1], space=zpeer(SP - 1)).start()

            @pl.when(has_below)
            def _():
                rcopy(own.at[pl.ds(8, 4)], own.at[pl.ds(0, 4)], hs.at[f, 1], hr.at[f, 0], space=zpeer(1)).start()

    def halo_took(f, sems):
        @pl.when(has_above)
        def _():
            took(xbuf.at[f, :, pl.ds(0, 4)], sems.at[f, 0])

        @pl.when(has_below)
        def _():
            took(xbuf.at[f, :, pl.ds(12, 4)], sems.at[f, 1])

    def project_own(f):
        xn[...] = norm_rows(xbuf[f, :, 4:12], gain1_ref[...])

        @unrolled(D // WIDE)
        def _(n):
            at = slice(n * WIDE, (n + 1) * WIDE)
            acc = jnp.dot(xn[...], w1[:, at], preferred_element_type=F32)
            qe[:, :, at] = (acc * even_mask).astype(BF16).reshape(TM, TB, WIDE)
            qo[:, :, at] = (acc * odd_mask).astype(BF16).reshape(TM, TB, WIDE)

        @unrolled(2 * D // WIDE)
        def _(n):
            at = slice(n * WIDE, (n + 1) * WIDE)
            wat = slice(n * WIDE + D, (n + 1) * WIDE + D)
            acc = jnp.dot(xn[...], w1[:, wat], preferred_element_type=F32)
            kv[:, HB : HB + TB, at] = acc.astype(BF16).reshape(TM, TB, WIDE)

    def project_halo(f):
        halo_took(f, hr)
        half = TM * HB
        xn[:half] = norm_rows(xbuf[f, :, :4], gain1_ref[...])
        xn[half:] = norm_rows(xbuf[f, :, 12:], gain1_ref[...])

        @unrolled(2 * D // WIDE)
        def _(n):
            at = slice(n * WIDE, (n + 1) * WIDE)
            wat = slice(n * WIDE + D, (n + 1) * WIDE + D)
            acc = jnp.dot(xn[...], w1[:, wat], preferred_element_type=F32).astype(BF16)
            kv[:, :HB, at] = acc[:half].reshape(TM, HB, WIDE)
            kv[:, HB + TB :, at] = acc[half:].reshape(TM, HB, WIDE)

    def attend_space(f, part):
        @pl.loop(0, 4 // GROUP)
        def _(m):
            places, chains = [], []
            for u in range(GROUP):
                first_col = (m * GROUP + u) * PAIR
                to = pl.ds(pl.multiple_of(first_col, PAIR), PAIR)
                at = pl.ds(pl.multiple_of(first_col + part * 512, PAIR), PAIR)
                vat = pl.ds(pl.multiple_of(first_col + part * 512 + D, PAIR), PAIR)
                for h in range(2):
                    rows = slice(h * HB, (h + 1) * HB)
                    keys = slice(h * HB, h * HB + 3 * HB)
                    q = [ref[:, rows, at].reshape(128, PAIR) for ref in (qe, qo)]
                    k = kv[:, keys, at].reshape(384, PAIR)
                    v = kv[:, keys, vat].reshape(384, PAIR)
                    places.append((rows, to))
                    chains.append((jnp.concatenate(q, axis=0), k, v, sbias[f, h]))
            for (rows, to), both in zip(places, attend(chains)):
                ctx[f, part, :, rows, to] = both.reshape(TM, HB, PAIR)

    def send_context(f, part):
        cbuf[f, part, me] = ctx[f, part, me]
        for d in range(1, TM):
            t = peer(d)
            rcopy(ctx.at[f, part, t], cbuf.at[f, part, me], ts.at[f, part], tr.at[f, part], tm=t).start()
        if f == 0:
            sent.append((ctx.at[f, part, pl.ds(0, TM - 1)], ts.at[f, part]))

    scope = jax.named_scope
    with scope("forward0"):
        forward(0, range(TM))
    with scope("w1_wait"):
        loads[0].wait()
    with scope("own0"):
        project_own(0)
        send_cotangent(0)
    with scope("halo0"):
        project_halo(0)
    with scope("forward1"):
        forward(1, range(6))
    with scope("attend0"):
        attend_space(0, 0)
        send_context(0, 0)
    with scope("forward1"):
        forward(1, (6, 7))
    with scope("attend0"):
        attend_space(0, 1)
        send_context(0, 1)
    with scope("own1"):
        project_own(1)
    with scope("halo1"):
        project_halo(1)
    with scope("attend1"):
        attend_space(1, 0)
        send_context(1, 0)
        attend_space(1, 1)
        send_context(1, 1)

    loads[1].wait()
    loads[2].wait()
    loads[3].wait()

    def merged(parts, tokens):
        joined = jnp.concatenate([parts[0], parts[1]], axis=-1).reshape(TM * TB, D)
        acc = jnp.dot(joined, m1[...], preferred_element_type=F32)
        return (acc + tokens.astype(F32).reshape(TM * TB, D)).astype(BF16)

    def merge(f):
        with scope("wait_ctx"):
            if f == 1:
                for part in range(2):
                    took(ctx.at[f, part, pl.ds(0, TM - 1)], ts.at[f, part])
                send_cotangent(1)
            for part in range(2):
                took(cbuf.at[f, part, pl.ds(0, TM - 1)], tr.at[f, part])

        with scope("merge"):
            mid[f] = merged((cbuf[f, 0], cbuf[f, 1]), xpos[:, f])
            xn2[...] = norm_rows(mid[f], gain2_ref[...])

        with scope("qkv2"):

            @unrolled(D // WIDE)
            def _(n):
                at = slice(n * WIDE, (n + 1) * WIDE)
                acc = jnp.dot(xn2[...], w2[:, at], preferred_element_type=F32)
                qe2[f, :, :, at] = (acc * even_mask).astype(BF16).reshape(TM, TB, WIDE)
                qo2[f, :, :, at] = (acc * odd_mask).astype(BF16).reshape(TM, TB, WIDE)

            @unrolled(2 * D // WIDE)
            def _(n):
                at = slice(n * WIDE, (n + 1) * WIDE)
                wat = slice(n * WIDE + D, (n + 1) * WIDE + D)
                acc = jnp.dot(xn2[...], w2[:, wat], preferred_element_type=F32)
                kv2[f, :, :, at] = acc.astype(BF16).reshape(TM, TB, WIDE)

    def temporal(g):
        places, chains = [], []
        for n in (2 * g, 2 * g + 1):
            at = slice(n * PAIR, (n + 1) * PAIR)
            vat = slice(n * PAIR + D, (n + 1) * PAIR + D)
            for b in range(2):
                rows = slice(b * 16, (b + 1) * 16)
                q = [ref[:, :, rows, at].reshape(256, PAIR) for ref in (qe2, qo2)]
                k = kv2[:, :, rows, at].reshape(256, PAIR)
                v = kv2[:, :, rows, vat].reshape(256, PAIR)
                places.append((rows, slice(n % 2 * PAIR, (n % 2 + 1) * PAIR)))
                chains.append((jnp.concatenate(q, axis=0), k, v, tbias[...]))
        for (rows, at), both in zip(places, attend(chains)):
            ctx2[g, :, :, rows, at] = both.reshape(FR, TM, 16, PAIR)

    first = []

    def gradient(g):
        a = ctx2[g].reshape(FR * TM * TB, 256)

        @unrolled(D // WIDE)
        def _(n):
            at = slice(n * WIDE, (n + 1) * WIDE)
            c = cotin[:, :, :, at].reshape(FR * TM * TB, WIDE)
            acc = lax.dot_general(a, c, (((0,), (0,)), ((), ())), preferred_element_type=F32)
            pbuf[g * 2 : g * 2 + 2, :, :, :, at] = acc.astype(BF16).reshape(2, SP, 2, 16, WIDE)

        cp = rcopy(
            pbuf.at[pl.ds(g * 2, 2), :, 1 - core], ra.at[pl.ds(g * 2, 2)], as_.at[g], ar.at[g], batch=mate
        )
        cp.start()
        first.append(cp)

    def reduce_core(g):
        with scope("reduce_core"):
            first[g].wait()
            rows = pl.ds(g * 2, 2)
            sa[rows] = (pbuf[rows, :, core].astype(F32) + ra[rows].astype(F32)).astype(BF16)
            for d in range(1, SP):
                rcopy(sa.at[rows, zpeer(d)], rb1.at[d - 1, rows], b1s.at[g], b1r.at[g], space=zpeer(d)).start()
            sent.append((sa.at[rows, pl.ds(0, SP - 1)], b1s.at[g]))

    def reduce_z(g):
        with scope("reduce_z"):
            rows = pl.ds(g * 2, 2)
            took(rb1.at[:, rows], b1r.at[g])
            total = sa[rows, z].astype(F32)
            for d in range(1, SP):
                total = total + rb1[d - 1, rows].astype(F32)
            sb1[rows] = total.astype(BF16)

    outs = []

    def output(f):
        joined = jnp.concatenate([ctx2[g, f].reshape(TM * TB, 256) for g in range(4)], axis=-1)
        acc = jnp.dot(joined, m2[...], preferred_element_type=F32) + mid[f].astype(F32)
        obuf[f] = acc.astype(BF16).reshape(TM, TB, D)
        cp = pltpu.make_async_copy(obuf.at[f, me], out_hbm.at[f, me], lsem.at[8 + f])
        cp.start()
        outs.append(cp)

    def send_output(f, start, count, i):
        rows = pl.ds(start, count)
        for d in range(1, TM):
            t = peer(d)
            rcopy(obuf.at[f, t, rows], out_hbm.at[f, me, rows], os_.at[i], or_.at[i], tm=t).start()
        whole = obuf.at[f, pl.ds(0, TM - 1), rows]
        sent.append((whole, os_.at[i]))
        sent.append((whole, or_.at[i]))

    merge(0)
    merge(1)
    for g in range(4):
        with scope("temporal"):
            temporal(g)
        if g == 0:
            loads[4].wait()
            with scope("wait_cot"):
                for f in range(FR):
                    cotin[f, me] = cot[f, me]
                    took(cotin.at[f, pl.ds(0, TM - 1)], cr.at[f])
        else:
            reduce_core(g - 1)
        with scope("gradient"):
            gradient(g)
    with scope("output0"):
        output(0)
        send_output(0, 0, TB, 0)
    reduce_core(3)
    with scope("output1"):
        output(1)
        send_output(1, 0, TB // 2, 1)

    for g in range(4):
        reduce_z(g)
    with scope("reduce_tm"):
        for d in range(1, TM):
            t = peer(d)
            rcopy(sb1.at[t], rb2.at[d - 1], b2s, b2r, tm=t).start()
        sent.append((sb1.at[pl.ds(0, TM - 1)], b2s))
        send_output(1, TB // 2, TB // 2, 2)
        took(rb2, b2r)
        total = sb1[me].astype(F32)
        for d in range(1, TM):
            total = total + rb2[d - 1].astype(F32)
        sb2[...] = total.astype(BF16)
    with scope("reduce_batch"):
        for i, other in enumerate(others):
            rcopy(sb2, rb3.at[i], b3s, b3r, batch=other).start()
        took(rb3, b3r)
        wg_ref[core] = sb2[...].astype(F32) + rb3[0].astype(F32)
        wg_ref[1 - core] = rb3[1].astype(F32) + rb3[2].astype(F32)

    with scope("wait_out"):
        took(rb3, b3s)
        took(tokens_sent, xs.at[1])
        halo_took(0, hs)
        halo_took(1, hs)
        for ref, sem in sent:
            took(ref, sem)
        for cp in outs:
            cp.wait()


def arrange(blocks_ref, grad_ref, out_ref, wg_ref):
    for k in range(2):
        halves = []
        for j in (2 * k, 2 * k + 1):
            a = blocks_ref[0, 2 * j].astype(F32).reshape(4, 8, D)
            b = blocks_ref[0, 2 * j + 1].astype(F32).reshape(4, 8, D)
            halves.append(exchange_halves(a, b))
        for i in range(2):
            rows = jnp.concatenate([halves[0][i], halves[1][i]], axis=1).astype(BF16)
            for r in range(4):
                out_ref[0, 2 * r + i, 16 * k : 16 * k + 16] = rows[r]
    wg_ref[...] = grad_ref[...]


def per_device(
    clip_tokens,
    frame_order,
    row_reach,
    spatial_gain,
    spatial_heads,
    spatial_merge,
    temporal_gain,
    temporal_heads,
    temporal_merge,
    cotangent,
):
    tokens = clip_tokens.reshape(TM, FR, 8, 4, D)
    grads = cotangent.reshape(FR, 8, 32, D)
    dma = pltpu.SemaphoreType.DMA
    vm = pltpu.VMEM
    smem = pl.BlockSpec(memory_space=pltpu.SMEM)
    vmem = pl.BlockSpec(memory_space=pltpu.VMEM)
    anym = pl.BlockSpec(memory_space=pl.ANY)
    blocks, grad = pl.pallas_call(
        kernel,
        out_shape=[
            jax.ShapeDtypeStruct((FR, TM, TB, D), BF16),
            jax.ShapeDtypeStruct((2, 16, D), F32),
        ],
        in_specs=[smem, smem, vmem, vmem] + [anym] * 6,
        out_specs=[anym, vmem],
        scratch_shapes=[
            vm((D, 3 * D), BF16),
            vm((D, D), BF16),
            vm((D, 3 * D), BF16),
            vm((D, D), BF16),
            vm((FR, TM, 16, 4, D), BF16),
            vm((TM * TB, D), BF16),
            vm((TM, TB, D), BF16),
            vm((TM, TB, D), BF16),
            vm((TM, EXT, 2 * D), BF16),
            vm((FR, 2, 384, 256), F32),
            vm((FR, 2, TM, TB, 512), BF16),
            vm((FR, 2, TM, TB, 512), BF16),
            vm((TM, FR, 8, 4, D), BF16),
            vm((FR, TM * TB, D), BF16),
            vm((TM * TB, D), BF16),
            vm((FR, TM, TB, D), BF16),
            vm((FR, TM, TB, D), BF16),
            vm((FR, TM, TB, 2 * D), BF16),
            vm((256, 512), F32),
            vm((4, FR, TM, TB, 256), BF16),
            vm((FR, 8, 32, D), BF16),
            vm((FR, TM, TB, D), BF16),
            vm((FR, TM, TB, D), BF16),
            vm((FR, TM, TB, D), BF16),
            vm((TM, SP, 2, 16, D), BF16),
            vm((TM, SP, 16, D), BF16),
            vm((TM, SP, 16, D), BF16),
            vm((SP - 1, TM, 16, D), BF16),
            vm((TM, 16, D), BF16),
            vm((TM - 1, 16, D), BF16),
            vm((16, D), BF16),
            vm((3, 16, D), BF16),
            dma((10,)),
            dma((FR,)),
            dma((FR, TM)),
            dma((FR, 2)),
            dma((FR, 2)),
            dma((FR, 2)),
            dma((FR, 2)),
            dma((FR,)),
            dma((FR,)),
            dma((3,)),
            dma((3,)),
            dma((4,)),
            dma((4,)),
            dma((4,)),
            dma((4,)),
            dma,
            dma,
            dma,
            dma,
        ],
        compiler_params=pltpu.CompilerParams(
            collective_id=0, has_side_effects=True, vmem_limit_bytes=62 * 1024 * 1024
        ),
    )(
        frame_order,
        row_reach,
        spatial_gain.reshape(1, D),
        temporal_gain.reshape(1, D),
        tokens,
        grads,
        spatial_heads,
        spatial_merge,
        temporal_heads,
        temporal_merge,
    )
    out, wg = pl.pallas_call(
        arrange,
        grid=(FR,),
        out_shape=[
            jax.ShapeDtypeStruct((FR, 8, 32, D), BF16),
            jax.ShapeDtypeStruct((2, 16, D), F32),
        ],
        in_specs=[
            pl.BlockSpec((1, TM, TB, D), lambda f: (f, 0, 0, 0)),
            pl.BlockSpec((2, 16, D), lambda f: (0, 0, 0)),
        ],
        out_specs=[
            pl.BlockSpec((1, 8, 32, D), lambda f: (f, 0, 0, 0)),
            pl.BlockSpec((2, 16, D), lambda f: (0, 0, 0)),
        ],
    )(blocks, grad)
    return out.reshape(1, FR, 8, 32, D), wg.reshape(32, D)


def solution(mesh):
    in_specs = (
        P("batch", None, "space", "tm", None),
        P("batch", None),
        P("batch", "tm"),
        P(),
        P(),
        P(),
        P(),
        P(),
        P(),
        P("batch", "tm", "space", None, None),
    )
    out_specs = (P("batch", "tm", "space", None, None), P(("tm", "space"), None))
    return jax.shard_map(
        per_device, mesh=mesh, in_specs=in_specs, out_specs=out_specs, check_vma=False
    )
```
